512 devices in a mesh: patch: 128 (over x, z, core), chan: 4 (over y).
Axes of the slice: x: 4, y: 4, z: 16, core: 2. Of those that a mesh axis runs over, the one named last changes fastest.
Arguments:
- grid_latent: bfloat16 [32768, 512], P('patch', 'chan'), may hold values from -6 to 6
- mesh_latent: bfloat16 [8192, 512], P('patch', 'chan'), may hold values from -6 to 6
- w_source: bfloat16 [512, 512], replicated, may hold values from -0.25 to 0.25
- w_dest: bfloat16 [512, 512], replicated, may hold values from -0.25 to 0.25
- w_out: bfloat16 [512, 512], replicated, may hold values from -0.25 to 0.25
- edge_bias: float32 [512], P('chan'), may hold values from -3 to 3
- norm_gain: float32 [512], P('chan'), may hold values from 0.5 to 1.5
- edge_source: int32 [65536], P('patch'), may hold values from 0 to 255
- edge_patch: int32 [65536, 1], P('patch'), may hold values from 0 to 127; in each aligned block of 512 rows (0 to 511, 512 to 1023, ...) at most 8 rows name the same one
- edge_node: int32 [65536], P('patch'), may hold values from 0 to 63
- cotangent: bfloat16 [8192, 512], P('patch', 'chan'), may hold values from -6 to 6
Outputs:
- updated: bfloat16 [8192, 512], P('patch', 'chan')
- grad_grid: bfloat16 [32768, 512], P('patch', 'chan')
- grad_mesh: bfloat16 [8192, 512], P('patch', 'chan')
- grad_w_source: float32 [512, 512], P(None, 'chan')
- grad_w_dest: float32 [512, 512], P(None, 'chan')
- grad_w_out: float32 [512, 512], P(None, 'chan')
- grad_bias: float32 [512], P('chan')
- grad_gain: float32 [512], P('chan')
The draws below stay inside these ranges and needn't reach their ends.
Inputs may be any that keep to these rules, and one draw needn't show every extreme that they name: `edge_patch`: the edges of band b are rows b * 512 to (b + 1) * 512 - 1; in the rows of one band no patch is named by more than 8 edges, and one patch is named by exactly 8.
All inputs are finite; a program needn't handle non-finite values.
Results may differ from the reference program's by a relative error of at most 0.0095.
Values may be sent and summed in bfloat16 or wider, within the bound.
No kernel may reach another device: no remote copies, remote signals or barrier semaphores. Data moves between devices by JAX's collectives and lax.ppermute only.
A program may use at most 64 MiB of HBM per device.

```python
import math
import jax
import jax.numpy as jnp
import numpy as np
from jax import lax

LATENT = 512
GRID_DEV = 256
EDGE_DEV = 512
MESH_DEV = 64
CAP = 8
GRID_NODES = 32768
MESH_NODES = 8192
EDGES = 65536
N_PATCH = 128


def place_ends(result, stream_key, least, top_value):
    dims = result.shape
    index_at = [jax.random.randint(jax.random.fold_in(stream_key, axis), (), 0, dims[axis]) for axis in range(len(dims))]
    result = result.at[tuple(index_at)].set(least)
    longest = dims.index(max(dims))
    index_at[longest] = (index_at[longest] + 1) % dims[longest]
    return result.at[tuple(index_at)].set(top_value)


def level_of(key, shape, shards, least, largest):
    factor_of, own = 1.0, jax.random.fold_in(key, 6)
    for position, shards_of in shards:
        draws = jnp.exp(jax.random.uniform(jax.random.fold_in(own, position), (shards_of,), jnp.float32, least / len(shards), largest / len(shards)))
        factor_of = factor_of * jnp.repeat(draws, shape[position] // shards_of).reshape([-1 if axis == position else 1 for axis in range(len(shape))])
    return factor_of


def shared_out(key, own, number, rows, number_of, top, most, skew):
    ranking = jax.random.permutation(key, number_of)
    crowded, usual = shares(number_of, rows * top, most, skew, True), shares(number_of, rows * top, most, skew, False)
    places = jnp.arange(number_of)

    def named(tallies, offset_by):
        used = int((tallies > 0).sum())
        fixed = max(1, used // 4)
        shifted = fixed + (places - fixed + offset_by * (used - fixed)) % max(1, number_of - fixed)
        return jnp.zeros((number_of,), jnp.int32).at[ranking[jnp.where(places < fixed, places, shifted)]].set(jnp.asarray(tallies, jnp.int32))

    tallies = jnp.where(number % 4 == 0, named(crowded, number // 4), named(usual, number - number // 4 - 1))
    mixed = jax.random.permutation(jax.random.fold_in(own, 3), number_of)
    donor, taker = mixed[0:number_of // 2 * 2:2], mixed[1:number_of // 2 * 2:2]
    margin = jnp.minimum(tallies[donor] - 1, most - tallies[taker]) // 2
    margin = jnp.where((donor == ranking[0]) | (taker == ranking[0]) | (tallies[taker] == 0), 0, jnp.maximum(margin, 0))
    shifted = jax.random.randint(jax.random.fold_in(own, 4), (number_of // 2,), 0, 1 << 20) % (margin + 1)
    tallies = tallies.at[donor].add(-shifted).at[taker].add(shifted)
    labels = jnp.searchsorted(jnp.cumsum(tallies), jnp.arange(rows * top), side="right").astype(jnp.int32)
    listing = labels.reshape(top, rows).T
    listing = listing[jax.random.permutation(jax.random.fold_in(own, 1), rows)]
    offset_by = jax.random.randint(jax.random.fold_in(own, 2), (rows, 1), 0, top)
    return jnp.take_along_axis(listing, (jnp.arange(top)[None, :] + offset_by) % top, axis=1)


def shares(amount, total, limit, slope, full):
    loads = [(1 << 20) // math.isqrt(rank ** slope) + 1 for rank in range(1, amount + 1)]
    largest = limit if full else min(limit, max(-(-total // amount), total * loads[0] // sum(loads)))
    least = 1 if total - largest >= amount - 1 else 0
    holding, spare = [largest] + [least] * (amount - 1), total - largest - least * (amount - 1)
    while spare > 0:
        free = [i for i in range(1, amount) if holding[i] < largest] or [i for i in range(1, amount) if holding[i] < limit]
        mass, remaining = sum([loads[i] for i in free]), spare
        for i in free:
            extra = min(limit - holding[i], max(1, remaining * loads[i] // mass), spare)
            holding[i] = holding[i] + extra
            spare = spare - extra
    return np.array(holding)


def gaussian(rng, dims, width, limit, split=(), kind=jnp.bfloat16):
    factor_of = level_of(rng, dims, split, -0.22, 0.18) if split else 1.0
    result = jax.random.normal(rng, dims, jnp.float32) * width * factor_of
    return jnp.minimum(jnp.maximum(result, -limit), limit).astype(kind)


def setup_inputs(seed: int = 0) -> dict:
    streams_of = jax.random.split(jax.random.key(seed), 12)
    grid_latent = gaussian(streams_of[0], (GRID_NODES, LATENT), 1.0, 6.0, ((0, 128), (1, 4)))
    mesh_latent = gaussian(streams_of[1], (MESH_NODES, LATENT), 1.0, 6.0, ((0, 128), (1, 4)))
    w_source = gaussian(streams_of[2], (LATENT, LATENT), LATENT ** -0.5, 0.25)
    w_dest = gaussian(streams_of[3], (LATENT, LATENT), LATENT ** -0.5, 0.25)
    w_out = gaussian(streams_of[4], (LATENT, LATENT), LATENT ** -0.5, 0.25)
    edge_bias = gaussian(streams_of[5], (LATENT,), 0.5, 3.0, ((0, 4),), jnp.float32)
    norm_gain = jnp.clip(1.0 + 0.1 * jax.random.normal(streams_of[6], (LATENT,), jnp.float32), 0.5, 1.5)
    edge_source = place_ends(jax.random.randint(streams_of[7], (EDGES,), 0, GRID_DEV), jax.random.fold_in(streams_of[7], 1), 0, GRID_DEV - 1).astype(jnp.int32)
    edge_patch_keys = jax.random.split(jax.random.fold_in(streams_of[8], 1), EDGES // EDGE_DEV)
    edge_patch_turns = jax.random.permutation(jax.random.fold_in(streams_of[8], 3), EDGES // EDGE_DEV)
    edge_patch = jax.vmap(lambda own, number: shared_out(jax.random.fold_in(streams_of[8], 2), own, number, EDGE_DEV, N_PATCH, 1, CAP, 2))(edge_patch_keys, edge_patch_turns).reshape((EDGES, 1))
    edge_node = place_ends(jax.random.randint(streams_of[9], (EDGES,), 0, MESH_DEV), jax.random.fold_in(streams_of[9], 1), 0, MESH_DEV - 1).astype(jnp.int32)
    cotangent = gaussian(streams_of[10], (MESH_NODES, LATENT), 1.0, 6.0, ((0, 128), (1, 4)))
    return dict(grid_latent=grid_latent, mesh_latent=mesh_latent, w_source=w_source, w_dest=w_dest, w_out=w_out, edge_bias=edge_bias, norm_gain=norm_gain, edge_source=edge_source, edge_patch=edge_patch, edge_node=edge_node, cotangent=cotangent)


norm_eps = 1e-05

def reference(grid_latent, mesh_latent, w_source, w_dest, w_out, edge_bias, norm_gain, edge_source, edge_patch, edge_node, cotangent):
    edge_total = edge_source.shape[0]
    band_index = (jnp.arange(edge_total, dtype=jnp.int32) // EDGE_DEV).astype(jnp.int32)
    src_row = (band_index * GRID_DEV + edge_source).astype(jnp.int32)
    dst_row = (edge_patch[:, 0] * MESH_DEV + edge_node).astype(jnp.int32)
    projected = jnp.dot(grid_latent, w_source, preferred_element_type=jnp.float32).astype(jnp.bfloat16)
    mesh_proj = jnp.dot(mesh_latent, w_dest, preferred_element_type=jnp.float32)
    pre_act = projected[src_row].astype(jnp.float32) + mesh_proj[dst_row] + edge_bias
    summed = jax.ops.segment_sum(jax.nn.silu(pre_act), dst_row, num_segments=MESH_NODES).astype(jnp.bfloat16)
    mixed = jnp.dot(summed, w_out, preferred_element_type=jnp.float32)
    row_mean = lax.optimization_barrier(jnp.mean(mixed, axis=1, keepdims=True))
    row_var = lax.optimization_barrier(jnp.mean(jnp.square(mixed - row_mean), axis=1, keepdims=True))
    inv_scale = lax.rsqrt(row_var + norm_eps)
    normed = (mixed - row_mean) * inv_scale
    updated = (mesh_latent.astype(jnp.float32) + normed * norm_gain).astype(jnp.bfloat16)
    cotan_full = cotangent.astype(jnp.float32)
    grad_gain = lax.optimization_barrier(jnp.sum(cotan_full * normed, axis=0))
    scaled = cotan_full * norm_gain
    grad_mixed = ((scaled - lax.optimization_barrier(jnp.mean(scaled, axis=1, keepdims=True)) - normed * lax.optimization_barrier(jnp.mean(scaled * normed, axis=1, keepdims=True))) * inv_scale).astype(jnp.bfloat16)
    grad_w_out = jnp.dot(summed.T, grad_mixed, preferred_element_type=jnp.float32)
    grad_summed = jnp.dot(grad_mixed, w_out.T, preferred_element_type=jnp.float32)
    sigmoid_val = jax.nn.sigmoid(pre_act)
    silu_slope = sigmoid_val * (1.0 + pre_act * (1.0 - sigmoid_val))
    grad_pre = (grad_summed[dst_row] * silu_slope).astype(jnp.bfloat16)
    grad_edges = grad_pre.astype(jnp.float32)
    grad_bias = lax.optimization_barrier(jnp.sum(grad_edges, axis=0))
    grad_mesh_proj = jax.ops.segment_sum(grad_edges, dst_row, num_segments=MESH_NODES).astype(jnp.bfloat16)
    grad_w_dest = jnp.dot(mesh_latent.T, grad_mesh_proj, preferred_element_type=jnp.float32)
    grad_mesh = (cotan_full + jnp.dot(grad_mesh_proj, w_dest.T, preferred_element_type=jnp.float32)).astype(jnp.bfloat16)
    grad_projected = jax.ops.segment_sum(grad_edges, src_row, num_segments=GRID_NODES).astype(jnp.bfloat16)
    grad_w_source = jnp.dot(grid_latent.T, grad_projected, preferred_element_type=jnp.float32)
    grad_grid = jnp.dot(grad_projected, w_source.T, preferred_element_type=jnp.float32).astype(jnp.bfloat16)
    return (updated, grad_grid, grad_mesh, grad_w_source, grad_w_dest, grad_w_out, grad_bias, grad_gain)
```

```python
import jax
import jax.numpy as jnp
from jax import lax
from jax.experimental import pallas as pl
from jax.sharding import Mesh
from jax.sharding import PartitionSpec as P

FAR = ("x", "z")
PATCH = ("x", "z", "c")
BF = jnp.bfloat16
F32 = jnp.float32

NORM_EPS = 1e-05
LANES = 128
CAP = 8
CHANS = 4
GRID = 256
MESH = 64
EDGES = 512
PATCHES = 128
LATENT = CHANS * LANES
SLOTS = PATCHES * CAP
HALF = CAP // 2 * LANES
COT_AT = GRID
MESH_AT = COT_AT + MESH
GAIN_AT = MESH_AT + MESH
PACK = GAIN_AT + 16
FARS = 64
WEIGHT_BLOCKS = LATENT // FARS
HALF_BLOCKS = 3 * WEIGHT_BLOCKS // 2
PARAM_COLS = (HALF_BLOCKS + 2) * LANES


def dot(a, b, dims=((1,), (0,))):
    return lax.dot_general(a, b, (dims, ((), ())), preferred_element_type=F32)


def two_parts(v):
    high = v.astype(BF)
    return high, (v - high.astype(F32)).astype(BF)


def iota(shape, dim):
    return lax.broadcasted_iota(jnp.int32, shape, dim)


def cols(j):
    return slice(j * LANES, (j + 1) * LANES)


def call(kernel, outs, args, flops):
    shapes = tuple(jax.ShapeDtypeStruct(s, d) for s, d in outs)
    return pl.pallas_call(
        kernel,
        out_shape=shapes,
        cost_estimate=pl.CostEstimate(flops=flops, bytes_accessed=1 << 20, transcendentals=0),
        name=kernel.__name__,
    )(*args)


def pack_kernel(grid, cot, mesh, gain, out):
    high, rest = two_parts(gain[...])
    left = gain[...] - high.astype(F32)
    low = left - rest.astype(F32)
    row = iota((16, LANES), 0)
    parts = jnp.where(
        row == 0,
        high.astype(F32),
        jnp.where(row == 1, rest.astype(F32), jnp.where(row == 2, low, 0.0)),
    )
    for j in range(CHANS):
        out[j, 0:GRID] = grid[...]
        out[j, COT_AT:MESH_AT] = cot[...]
        out[j, MESH_AT:GAIN_AT] = mesh[...]
        out[j, GAIN_AT:PACK] = parts.astype(BF)


def slot_kernel(patch_col, patch_row, source, node, pick, meta):
    before = iota((EDGES, EDGES), 0) < iota((EDGES, EDGES), 1)
    same = patch_col[...] == patch_row[...]
    rank = jnp.sum(jnp.where(same & before, 1.0, 0.0), axis=0, keepdims=True)
    slot = rank.astype(jnp.int32) * PATCHES + patch_row[...]
    here = jnp.where(iota((SLOTS, EDGES), 0) == slot, 1.0, 0.0).astype(BF)
    row = iota((8, EDGES), 0)
    facts = jnp.where(
        row == 0, source[...], jnp.where(row == 1, node[...], jnp.where(row == 2, 1, 0))
    )
    found = dot(here, facts.astype(F32).astype(BF), ((1,), (1,)))
    live = found[:, 2:3] > 0.5
    from_row = jnp.where(live, found[:, 0:1], -1.0).astype(jnp.int32)
    pick[...] = jnp.where(iota((SLOTS, GRID), 1) == from_row, 1.0, 0.0).astype(BF)
    to_node = jnp.where(live, found[:, 1:2], float(MESH))
    lane = iota((PATCHES, LANES), 1)
    listed = jnp.zeros((PATCHES, LANES), F32)
    for r in range(CAP):
        listed = jnp.where(lane == r, to_node[r * PATCHES : (r + 1) * PATCHES], listed)
    meta[...] = listed.astype(BF)


def slot_at(r):
    at = r // (CAP // 2) * (HALF + LANES) + r % (CAP // 2) * LANES
    return slice(at, at + LANES)


def send_kernel(packed, pick, meta, source_cols, dest_cols, out, mesh_proj):
    projected = jnp.zeros((GRID, LANES), F32)
    landed = jnp.zeros((MESH, LANES), F32)
    for j in range(CHANS):
        projected += dot(packed[j, 0:GRID], source_cols[cols(j)])
        landed += dot(packed[j, MESH_AT:GAIN_AT], dest_cols[cols(j)])
    mesh_proj[...] = landed
    projected = projected.astype(BF)
    for r in range(CAP):
        rows = pick[r * PATCHES : (r + 1) * PATCHES]
        out[:, slot_at(r)] = dot(rows, projected).astype(BF)
    out[:, HALF : HALF + LANES] = meta[...]
    out[:, 2 * HALF + LANES : 2 * HALF + 2 * LANES] = jnp.zeros((PATCHES, LANES), BF)


def message_kernel(arrived, mesh_proj, bias, summed, pre, chosen):
    high, low = two_parts(mesh_proj[...])
    both = jnp.concatenate([high, low], axis=1)
    total = jnp.zeros((MESH, 2 * LANES), F32)
    for r in range(CAP):
        at = slice(r * PATCHES, (r + 1) * PATCHES)
        node = arrived[:, HALF + r : HALF + r + 1].astype(F32).astype(jnp.int32)
        mine = jnp.where(iota((PATCHES, MESH), 1) == node, 1.0, 0.0).astype(BF)
        chosen[at] = mine
        there = dot(mine, both)
        value = (
            arrived[:, slot_at(r)].astype(F32)
            + (there[:, 0:LANES] + there[:, LANES : 2 * LANES])
            + bias[...]
        )
        pre[at] = value
        message = value * jax.nn.sigmoid(value)
        total += dot(mine, jnp.concatenate(two_parts(message), axis=1), ((0,), (0,)))
    done = (total[:, 0:LANES] + total[:, LANES : 2 * LANES]).astype(BF)
    for j in range(CHANS):
        summed[j] = done


def node_kernel(
    packed,
    summed,
    pre,
    chosen,
    w_out,
    out_cols,
    out_rows,
    mesh,
    cot,
    gain,
    updated,
    grads,
    node_grad,
    dest_part,
    out_part,
    bias_part,
    gain_part,
):
    mixed = jnp.zeros((MESH, LATENT), F32)
    own = jnp.zeros((MESH, LANES), F32)
    for j in range(CHANS):
        mixed += dot(summed[j], w_out[cols(j)])
        own += dot(summed[j], out_cols[cols(j)])
    mean = jnp.sum(mixed, axis=1, keepdims=True) / LATENT
    apart = mixed - mean
    inv = lax.rsqrt(jnp.sum(apart * apart, axis=1, keepdims=True) / LATENT + NORM_EPS)
    normed = apart * inv
    scaled, first, second = [], 0.0, 0.0
    for j in range(CHANS):
        parts = packed[j, GAIN_AT:PACK].astype(F32)
        whole = parts[0:1] + parts[1:2] + parts[2:3]
        part = packed[j, COT_AT:MESH_AT].astype(F32) * whole
        scaled.append(part)
        first += jnp.sum(part, axis=1, keepdims=True)
        second += jnp.sum(part * normed[:, cols(j)], axis=1, keepdims=True)
    first, second = first / LATENT, second / LATENT
    own_normed = (own - mean) * inv
    cotangent = cot[...].astype(F32)
    updated[...] = (mesh[...].astype(F32) + own_normed * gain[...]).astype(BF)
    gain_part[...] = jnp.sum(cotangent * own_normed, axis=0, keepdims=True)
    own_grad = ((cotangent * gain[...] - first - own_normed * second) * inv).astype(BF)
    back = jnp.zeros((MESH, LANES), F32)
    for j in range(CHANS):
        out_part[cols(j)] = dot(summed[j], own_grad, ((0,), (0,))).astype(BF)
        part = ((scaled[j] - first - normed[:, cols(j)] * second) * inv).astype(BF)
        back += dot(part, out_rows[:, cols(j)], ((1,), (1,)))
    both = jnp.concatenate(two_parts(back), axis=1)
    bias = jnp.zeros((1, LANES), F32)
    total = jnp.zeros((MESH, LANES), F32)
    for r in range(CAP):
        at = slice(r * PATCHES, (r + 1) * PATCHES)
        mine = chosen[at]
        there = dot(mine, both)
        value = pre[at]
        gate = jax.nn.sigmoid(value)
        slope = gate * (1.0 + value * (1.0 - gate))
        grad = ((there[:, 0:LANES] + there[:, LANES : 2 * LANES]) * slope).astype(BF)
        grads[:, cols(r)] = grad
        bias += jnp.sum(grad.astype(F32), axis=0, keepdims=True)
        total += dot(mine, grad, ((0,), (0,)))
    bias_part[...] = bias
    total = total.astype(BF)
    node_grad[...] = total
    for j in range(CHANS):
        dest_part[cols(j)] = dot(packed[j, MESH_AT:GAIN_AT], total, ((0,), (0,))).astype(BF)


def grid_kernel(
    returned, pick, packed, node_grad, dest_part, out_part, bias_part, gain_part, out, params
):
    total = jnp.zeros((GRID, LANES), F32)
    for r in range(CAP):
        rows = pick[r * PATCHES : (r + 1) * PATCHES]
        total += dot(rows, returned[:, cols(r)], ((0,), (0,)))
    total = total.astype(BF)
    for j in range(CHANS):
        out[j, 0:GRID] = total
        out[j, GRID : GRID + MESH] = node_grad[...]
    blocks = []
    for j in range(CHANS):
        part = dot(packed[j, 0:GRID], total, ((0,), (0,))).astype(BF)
        blocks += [part[0:FARS], part[FARS : 2 * FARS]]
    for whole in (dest_part, out_part):
        blocks += [whole[b * FARS : (b + 1) * FARS] for b in range(WEIGHT_BLOCKS)]
    for b, block in enumerate(blocks):
        params[b // HALF_BLOCKS, :, cols(b % HALF_BLOCKS)] = block
    head = iota((FARS, LANES), 0) == 0
    for half, small in enumerate((bias_part, gain_part)):
        for k, part in enumerate(two_parts(small[...])):
            spread = jnp.where(head, part.astype(F32), 0.0)
            params[half, :, cols(HALF_BLOCKS + k)] = spread.astype(BF)


def back_kernel(gathered, source_rows, dest_rows, cot, grad_grid, grad_mesh):
    on_grid = jnp.zeros((GRID, LANES), F32)
    on_mesh = cot[...].astype(F32)
    for j in range(CHANS):
        on_grid += dot(gathered[j, 0:GRID], source_rows[:, cols(j)], ((1,), (1,)))
        on_mesh += dot(gathered[j, GRID : GRID + MESH], dest_rows[:, cols(j)], ((1,), (1,)))
    grad_grid[...] = on_grid.astype(BF)
    grad_mesh[...] = on_mesh.astype(BF)


def pair_kernel(params, out):
    total = params[0].astype(F32) + params[1].astype(F32)
    small = total[:, cols(HALF_BLOCKS)] + total[:, cols(HALF_BLOCKS + 1)]
    out[:, 0 : HALF_BLOCKS * LANES] = total[:, 0 : HALF_BLOCKS * LANES].astype(BF)
    for k, part in enumerate(two_parts(small)):
        out[:, cols(HALF_BLOCKS + k)] = part


def unpack_kernel(params, source, dest, out, bias, gain):
    for b in range(3 * WEIGHT_BLOCKS):
        block = params[b // HALF_BLOCKS, :, cols(b % HALF_BLOCKS)].astype(F32)
        at = b % WEIGHT_BLOCKS * FARS
        (source, dest, out)[b // WEIGHT_BLOCKS][at : at + FARS] = block
    for half, small in enumerate((bias, gain)):
        high = params[half, 0:1, cols(HALF_BLOCKS)].astype(F32)
        small[...] = high + params[half, 0:1, cols(HALF_BLOCKS + 1)].astype(F32)


def gather_stage(st):
    args = (st["grid_latent"], st["cotangent"], st["mesh_latent"], st["norm_gain"][None])
    (st["sent"],) = call(pack_kernel, [((CHANS, PACK, LANES), BF)], args, 1 << 20)
    return st


def send_stage(st):
    offset = st["chan"] * LANES
    st["packed"] = st["got"]
    for name in ("source", "dest", "out"):
        whole = st["w_" + name]
        st[name + "_cols"] = lax.dynamic_slice_in_dim(whole, offset, LANES, 1)
        st[name + "_rows"] = lax.dynamic_slice_in_dim(whole, offset, LANES, 0)
    patch = st["edge_patch"]
    args = (patch, patch.reshape(1, EDGES), st["edge_source"][None], st["edge_node"][None])
    outs = [((SLOTS, GRID), BF), ((PATCHES, LANES), BF)]
    st["pick"], meta = call(slot_kernel, outs, args, 1 << 27)
    args = (st["packed"], st["pick"], meta, st["source_cols"], st["dest_cols"])
    outs = [((PATCHES, 2 * HALF + 2 * LANES), BF), ((MESH, LANES), F32)]
    sent, st["mesh_proj"] = call(send_kernel, outs, args, 1 << 28)
    st["sent"] = sent.reshape(PATCHES, 2, HALF + LANES)
    return st


def message_stage(st):
    arrived = st["got"].reshape(PATCHES, 2 * HALF + 2 * LANES)
    outs = [((CHANS, MESH, LANES), BF), ((SLOTS, LANES), F32), ((SLOTS, MESH), BF)]
    args = (arrived, st["mesh_proj"], st["edge_bias"][None])
    st["sent"], st["pre"], st["chosen"] = call(message_kernel, outs, args, 1 << 27)
    return st


def node_stage(st):
    args = [st["packed"], st["got"], st["pre"], st["chosen"], st["w_out"], st["out_cols"]]
    args += [st["out_rows"], st["mesh_latent"], st["cotangent"], st["norm_gain"][None]]
    outs = [((MESH, LANES), BF), ((PATCHES, 2 * HALF), BF), ((MESH, LANES), BF)]
    outs += [((LATENT, LANES), BF)] * 2 + [((1, LANES), F32)] * 2
    st["updated"], grads, *st["partial"] = call(node_kernel, outs, args, 1 << 28)
    st["sent"] = grads.reshape(PATCHES, 2, HALF)
    return st


def grid_stage(st):
    returned = st["got"].reshape(PATCHES, 2 * HALF)
    outs = [((CHANS, GRID + MESH, LANES), BF), ((2, FARS, PARAM_COLS), BF)]
    args = (returned, st["pick"], st["packed"], *st["partial"])
    st["sent"], st["params"] = call(grid_kernel, outs, args, 1 << 28)
    return st


def back_stage(st):
    args = (st["got"], st["source_rows"], st["dest_rows"], st["cotangent"])
    outs = [((GRID, LANES), BF), ((MESH, LANES), BF)]
    st["grad_grid"], st["grad_mesh"] = call(back_kernel, outs, args, 1 << 26)
    st["sent"] = st["params"]
    return st


def far_stage(st):
    (sent,) = call(pair_kernel, [((FARS, PARAM_COLS), BF)], (st["got"],), 1 << 18)
    st["sent"] = sent.reshape(FARS, 2, PARAM_COLS // 2)
    return st


def sum_stage(st):
    total = jnp.sum(st["got"].astype(F32), axis=0)
    at = PARAM_COLS // 2 - 2 * LANES
    small = total[1:2, at : at + LANES] + total[1:2, at + LANES :]
    high = lax.reduce_precision(small, 8, 7)
    last = jnp.concatenate([total[1:2, :at], high, small - high], axis=1)
    total = jnp.concatenate([total[0:1], last], axis=0).astype(BF)
    st["sent"] = jnp.broadcast_to(total, (FARS, 2, PARAM_COLS // 2))
    return st


def near_stage(st):
    whole = st["got"].reshape(FARS, PARAM_COLS)
    st["sent"] = jnp.broadcast_to(whole, (2, FARS, PARAM_COLS))
    return st


def last_stage(st):
    outs = [((LATENT, LANES), F32)] * 3 + [((1, LANES), F32)] * 2
    *weights, bias, gain = call(unpack_kernel, outs, (st["got"],), 1 << 18)
    st["params"] = (*weights, bias.reshape(LANES), gain.reshape(LANES))
    return st


STAGES = (
    (gather_stage, "y"),
    (send_stage, PATCH),
    (message_stage, "y"),
    (node_stage, PATCH),
    (grid_stage, "y"),
    (back_stage, "c"),
    (far_stage, FAR),
    (sum_stage, FAR),
    (near_stage, "c"),
    (last_stage, None),
)

NAMES = (
    "grid_latent",
    "mesh_latent",
    "w_source",
    "w_dest",
    "w_out",
    "edge_bias",
    "norm_gain",
    "edge_source",
    "edge_patch",
    "edge_node",
    "cotangent",
)


def on_device(*args):
    st = dict(zip(NAMES, args))
    st["chan"] = lax.axis_index("y")
    for stage, axes in STAGES:
        st = stage(st)
        if axes is not None:
            st["got"] = lax.all_to_all(st["sent"], axes, 0, 0, tiled=True)
    return (st["updated"], st["grad_grid"], st["grad_mesh"], *st["params"])


def solution(mesh):
    torus = Mesh(mesh.devices.reshape(4, 16, 2, mesh.shape["chan"]), ("x", "z", "c", "y"))
    by_patch = P(PATCH, "y")
    return jax.shard_map(
        on_device,
        mesh=torus,
        in_specs=(by_patch, by_patch, P(), P(), P(), P("y"), P("y"))
        + (P(PATCH), P(PATCH, None), P(PATCH), by_patch),
        out_specs=(by_patch,) * 3 + (P(None, "y"),) * 3 + (P("y"),) * 2,
        check_vma=False,
    )
```

```python
import jax
import jax.numpy as jnp
from jax import lax
from jax.experimental import pallas as pl
from jax.experimental.pallas import tpu as pltpu
from jax.sharding import Mesh
from jax.sharding import PartitionSpec as P


NEAR = ("x", "c")
PATCH = ("x", "z", "c")
BF = jnp.bfloat16
F32 = jnp.float32

NORM_EPS = 1e-05
LANES = 128
CAP = 8
CHANS = 4
GRID = 256
MESH = 64
EDGES = 512
PATCHES = 128
LATENT = CHANS * LANES
SLOTS = PATCHES * CAP
HALF = CAP // 2 * LANES
COT_AT = GRID
MESH_AT = COT_AT + MESH
GAIN_AT = MESH_AT + MESH
PACK = GAIN_AT + 16
NEARS = 8
FARS = 16
WEIGHT_BLOCKS = LATENT // FARS
OWN_BLOCKS = 3 * WEIGHT_BLOCKS // NEARS
PARAM_COLS = (OWN_BLOCKS + 2) * LANES
VMEM_BYTES = 20 << 20


def dot(a, b, dims=((1,), (0,))):
    return lax.dot_general(a, b, (dims, ((), ())), preferred_element_type=F32)


def two_parts(v):
    high = v.astype(BF)
    return high, (v - high.astype(F32)).astype(BF)


def iota(shape, dim):
    return lax.broadcasted_iota(jnp.int32, shape, dim)


def cols(j):
    return slice(j * LANES, (j + 1) * LANES)


def call(kernel, outs, args, flops, **more):
    shapes = tuple(jax.ShapeDtypeStruct(s, d) for s, d in outs)
    return pl.pallas_call(
        kernel,
        out_shape=shapes,
        compiler_params=pltpu.CompilerParams(vmem_limit_bytes=VMEM_BYTES),
        **more,
        cost_estimate=pl.CostEstimate(flops=flops, bytes_accessed=1 << 20, transcendentals=0),
    )(*args)


def pack_kernel(grid, cot, mesh, gain, out):
    high, rest = two_parts(gain[...])
    left = gain[...] - high.astype(F32)
    low = left - rest.astype(F32)
    row = iota((16, LANES), 0)
    parts = jnp.where(
        row == 0,
        high.astype(F32),
        jnp.where(row == 1, rest.astype(F32), jnp.where(row == 2, low, 0.0)),
    )
    for j in range(CHANS):
        out[j, 0:GRID] = grid[...]
        out[j, COT_AT:MESH_AT] = cot[...]
        out[j, MESH_AT:GAIN_AT] = mesh[...]
        out[j, GAIN_AT:PACK] = parts.astype(BF)


def slot_kernel(patch_col, patch_row, source, node, pick, meta):
    before = iota((EDGES, EDGES), 0) < iota((EDGES, EDGES), 1)
    same = patch_col[...] == patch_row[...]
    rank = jnp.sum(jnp.where(same & before, 1.0, 0.0), axis=0, keepdims=True)
    slot = rank.astype(jnp.int32) * PATCHES + patch_row[...]
    here = jnp.where(iota((SLOTS, EDGES), 0) == slot, 1.0, 0.0).astype(BF)
    row = iota((8, EDGES), 0)
    facts = jnp.where(
        row == 0, source[...], jnp.where(row == 1, node[...], jnp.where(row == 2, 1, 0))
    )
    found = dot(here, facts.astype(F32).astype(BF), ((1,), (1,)))
    live = found[:, 2:3] > 0.5
    from_row = jnp.where(live, found[:, 0:1], -1.0).astype(jnp.int32)
    pick[...] = jnp.where(iota((SLOTS, GRID), 1) == from_row, 1.0, 0.0).astype(BF)
    to_node = jnp.where(live, found[:, 1:2], float(MESH))
    lane = iota((PATCHES, LANES), 1)
    listed = jnp.zeros((PATCHES, LANES), F32)
    for r in range(CAP):
        listed = jnp.where(lane == r, to_node[r * PATCHES : (r + 1) * PATCHES], listed)
    meta[...] = listed.astype(BF)


def slot_at(r):
    at = r // (CAP // 2) * (HALF + LANES) + r % (CAP // 2) * LANES
    return slice(at, at + LANES)


def send_kernel(packed, pick, meta, source_cols, dest_cols, out, mesh_proj):
    projected = jnp.zeros((GRID, LANES), F32)
    landed = jnp.zeros((MESH, LANES), F32)
    for j in range(CHANS):
        projected += dot(packed[j, 0:GRID], source_cols[cols(j)])
        landed += dot(packed[j, MESH_AT:GAIN_AT], dest_cols[cols(j)])
    mesh_proj[...] = landed
    projected = projected.astype(BF)
    for r in range(CAP):
        rows = pick[r * PATCHES : (r + 1) * PATCHES]
        out[:, slot_at(r)] = dot(rows, projected).astype(BF)
    out[:, HALF : HALF + LANES] = meta[...]
    out[:, 2 * HALF + LANES : 2 * HALF + 2 * LANES] = jnp.zeros((PATCHES, LANES), BF)


def message_kernel(arrived, mesh_proj, bias, summed, pre, chosen):
    high, low = two_parts(mesh_proj[...])
    both = jnp.concatenate([high, low], axis=1)
    total = jnp.zeros((MESH, 2 * LANES), F32)
    for r in range(CAP):
        at = slice(r * PATCHES, (r + 1) * PATCHES)
        node = arrived[:, HALF + r : HALF + r + 1].astype(F32).astype(jnp.int32)
        mine = jnp.where(iota((PATCHES, MESH), 1) == node, 1.0, 0.0).astype(BF)
        chosen[at] = mine
        there = dot(mine, both)
        value = (
            arrived[:, slot_at(r)].astype(F32)
            + (there[:, 0:LANES] + there[:, LANES : 2 * LANES])
            + bias[...]
        )
        pre[at] = value
        message = value * jax.nn.sigmoid(value)
        total += dot(mine, jnp.concatenate(two_parts(message), axis=1), ((0,), (0,)))
    done = (total[:, 0:LANES] + total[:, LANES : 2 * LANES]).astype(BF)
    for j in range(CHANS):
        summed[j] = done


def node_kernel(
    packed,
    summed,
    pre,
    chosen,
    w_out,
    out_cols,
    out_rows,
    mesh,
    cot,
    gain,
    updated,
    grads,
    node_grad,
    dest_part,
    out_part,
    bias_part,
    gain_part,
):
    mixed = jnp.zeros((MESH, LATENT), F32)
    own = jnp.zeros((MESH, LANES), F32)
    for j in range(CHANS):
        mixed += dot(summed[j], w_out[cols(j)])
        own += dot(summed[j], out_cols[cols(j)])
    mean = jnp.sum(mixed, axis=1, keepdims=True) / LATENT
    apart = mixed - mean
    inv = lax.rsqrt(jnp.sum(apart * apart, axis=1, keepdims=True) / LATENT + NORM_EPS)
    normed = apart * inv
    scaled, first, second = [], 0.0, 0.0
    for j in range(CHANS):
        parts = packed[j, GAIN_AT:PACK].astype(F32)
        whole = parts[0:1] + parts[1:2] + parts[2:3]
        part = packed[j, COT_AT:MESH_AT].astype(F32) * whole
        scaled.append(part)
        first += jnp.sum(part, axis=1, keepdims=True)
        second += jnp.sum(part * normed[:, cols(j)], axis=1, keepdims=True)
    first, second = first / LATENT, second / LATENT
    own_normed = (own - mean) * inv
    cotangent = cot[...].astype(F32)
    updated[...] = (mesh[...].astype(F32) + own_normed * gain[...]).astype(BF)
    gain_part[...] = jnp.sum(cotangent * own_normed, axis=0, keepdims=True)
    own_grad = ((cotangent * gain[...] - first - own_normed * second) * inv).astype(BF)
    back = jnp.zeros((MESH, LANES), F32)
    for j in range(CHANS):
        out_part[cols(j)] = dot(summed[j], own_grad, ((0,), (0,))).astype(BF)
        part = ((scaled[j] - first - normed[:, cols(j)] * second) * inv).astype(BF)
        back += dot(part, out_rows[:, cols(j)], ((1,), (1,)))
    both = jnp.concatenate(two_parts(back), axis=1)
    bias = jnp.zeros((1, LANES), F32)
    total = jnp.zeros((MESH, LANES), F32)
    for r in range(CAP):
        at = slice(r * PATCHES, (r + 1) * PATCHES)
        mine = chosen[at]
        there = dot(mine, both)
        value = pre[at]
        gate = jax.nn.sigmoid(value)
        slope = gate * (1.0 + value * (1.0 - gate))
        grad = ((there[:, 0:LANES] + there[:, LANES : 2 * LANES]) * slope).astype(BF)
        grads[:, cols(r)] = grad
        bias += jnp.sum(grad.astype(F32), axis=0, keepdims=True)
        total += dot(mine, grad, ((0,), (0,)))
    bias_part[...] = bias
    total = total.astype(BF)
    node_grad[...] = total
    for j in range(CHANS):
        dest_part[cols(j)] = dot(packed[j, MESH_AT:GAIN_AT], total, ((0,), (0,))).astype(BF)


def grid_kernel(
    returned, pick, packed, node_grad, dest_part, out_part, bias_part, gain_part, out, params
):
    total = jnp.zeros((GRID, LANES), F32)
    for r in range(CAP):
        rows = pick[r * PATCHES : (r + 1) * PATCHES]
        total += dot(rows, returned[:, cols(r)], ((0,), (0,)))
    total = total.astype(BF)
    out[0:GRID] = total
    out[GRID : GRID + MESH] = node_grad[...]
    blocks = []
    for j in range(CHANS):
        part = dot(packed[j, 0:GRID], total, ((0,), (0,))).astype(BF)
        blocks += [part[b * FARS : (b + 1) * FARS] for b in range(LANES // FARS)]
    for whole in (dest_part, out_part):
        blocks += [whole[b * FARS : (b + 1) * FARS] for b in range(WEIGHT_BLOCKS)]
    for b, block in enumerate(blocks):
        params[b // OWN_BLOCKS, :, cols(b % OWN_BLOCKS)] = block
    head = iota((FARS, LANES), 0) == 0
    small = [bias_part[...], gain_part[...]] + [jnp.zeros((1, LANES), F32)] * (NEARS - 2)
    for g in range(NEARS):
        for k, part in enumerate(two_parts(small[g])):
            spread = jnp.where(head, part.astype(F32), 0.0)
            params[g, :, cols(OWN_BLOCKS + k)] = spread.astype(BF)


def back_kernel(
    chan, own, last, middle, following, source_rows, dest_rows, cot, grad_grid, grad_mesh
):
    on_grid = jnp.zeros((GRID, LANES), F32)
    on_mesh = cot[...].astype(F32)
    for k, block in enumerate((own, last, middle, following)):
        at = pl.multiple_of(lax.rem(chan[0] + CHANS - k, CHANS) * LANES, LANES)
        there = pl.ds(at, LANES)
        on_grid += dot(block[0:GRID], source_rows[:, there], ((1,), (1,)))
        on_mesh += dot(block[GRID : GRID + MESH], dest_rows[:, there], ((1,), (1,)))
    grad_grid[...] = on_grid.astype(BF)
    grad_mesh[...] = on_mesh.astype(BF)


def near_sum_kernel(params, out):
    total = params[0].astype(F32)
    for g in range(1, NEARS):
        total += params[g].astype(F32)
    small = total[:, cols(OWN_BLOCKS)] + total[:, cols(OWN_BLOCKS + 1)]
    out[:, 0 : OWN_BLOCKS * LANES] = total[:, 0 : OWN_BLOCKS * LANES].astype(BF)
    for k, part in enumerate(two_parts(small)):
        out[:, cols(OWN_BLOCKS + k)] = part


def unpack_kernel(params, source, dest, out, bias, gain):
    for b in range(3 * WEIGHT_BLOCKS):
        block = params[b // OWN_BLOCKS, :, cols(b % OWN_BLOCKS)].astype(F32)
        at = b % WEIGHT_BLOCKS * FARS
        (source, dest, out)[b // WEIGHT_BLOCKS][at : at + FARS] = block
    for g, small in enumerate((bias, gain)):
        high = params[g, 0:1, cols(OWN_BLOCKS)].astype(F32)
        small[...] = high + params[g, 0:1, cols(OWN_BLOCKS + 1)].astype(F32)


def gather_stage(st):
    args = (st["grid_latent"], st["cotangent"], st["mesh_latent"], st["norm_gain"][None])
    (st["sent"],) = call(pack_kernel, [((CHANS, PACK, LANES), BF)], args, 1 << 20)
    return st


def send_stage(st):
    offset = st["chan"] * LANES
    st["packed"] = st["got"]
    for name in ("source", "dest", "out"):
        whole = st["w_" + name]
        st[name + "_cols"] = lax.dynamic_slice_in_dim(whole, offset, LANES, 1)
        st[name + "_rows"] = lax.dynamic_slice_in_dim(whole, offset, LANES, 0)
    patch = st["edge_patch"]
    args = (patch, patch.reshape(1, EDGES), st["edge_source"][None], st["edge_node"][None])
    outs = [((SLOTS, GRID), BF), ((PATCHES, LANES), BF)]
    st["pick"], meta = call(slot_kernel, outs, args, 1 << 27)
    args = (st["packed"], st["pick"], meta, st["source_cols"], st["dest_cols"])
    outs = [((PATCHES, 2 * HALF + 2 * LANES), BF), ((MESH, LANES), F32)]
    sent, st["mesh_proj"] = call(send_kernel, outs, args, 1 << 28)
    st["sent"] = sent.reshape(PATCHES, 2, HALF + LANES)
    return st


def message_stage(st):
    arrived = st["got"].reshape(PATCHES, 2 * HALF + 2 * LANES)
    outs = [((CHANS, MESH, LANES), BF), ((SLOTS, LANES), F32), ((SLOTS, MESH), BF)]
    args = (arrived, st["mesh_proj"], st["edge_bias"][None])
    st["sent"], st["pre"], st["chosen"] = call(message_kernel, outs, args, 1 << 27)
    return st


def node_stage(st):
    args = [st["packed"], st["got"], st["pre"], st["chosen"], st["w_out"], st["out_cols"]]
    args += [st["out_rows"], st["mesh_latent"], st["cotangent"], st["norm_gain"][None]]
    outs = [((MESH, LANES), BF), ((PATCHES, 2 * HALF), BF), ((MESH, LANES), BF)]
    outs += [((LATENT, LANES), BF)] * 2 + [((1, LANES), F32)] * 2
    st["updated"], grads, *st["partial"] = call(node_kernel, outs, args, 1 << 28)
    st["sent"] = grads.reshape(PATCHES, 2, HALF)
    return st


def grid_stage(st):
    returned = st["got"].reshape(PATCHES, 2 * HALF)
    outs = [((GRID + MESH, LANES), BF), ((NEARS, FARS, PARAM_COLS), BF)]
    args = (returned, st["pick"], st["packed"], *st["partial"])
    st["sent"], st["params"] = call(grid_kernel, outs, args, 1 << 28)
    return st


def back_stage(st):
    args = (st["chan"][None], *st["got"], st["source_rows"], st["dest_rows"], st["cotangent"])
    outs = [((GRID, LANES), BF), ((MESH, LANES), BF)]
    specs = [pl.BlockSpec(memory_space=pltpu.SMEM)] + [pl.BlockSpec()] * (len(args) - 1)
    st["grad_grid"], st["grad_mesh"] = call(back_kernel, outs, args, 1 << 26, in_specs=specs)
    st["sent"] = st["params"]
    return st


def far_stage(st):
    (sent,) = call(near_sum_kernel, [((FARS, PARAM_COLS), BF)], (st["got"],), 1 << 18)
    st["sent"] = sent.reshape(FARS, 2, PARAM_COLS // 2)
    return st


def sum_stage(st):
    total = jnp.sum(st["got"].astype(F32), axis=0)
    at = PARAM_COLS // 2 - 2 * LANES
    small = total[1:2, at : at + LANES] + total[1:2, at + LANES :]
    high = lax.reduce_precision(small, 8, 7)
    last = jnp.concatenate([total[1:2, :at], high, small - high], axis=1)
    total = jnp.concatenate([total[0:1], last], axis=0).astype(BF)
    st["sent"] = jnp.broadcast_to(total, (FARS, 2, PARAM_COLS // 2))
    return st


def near_stage(st):
    whole = st["got"].reshape(FARS, PARAM_COLS)
    st["sent"] = jnp.broadcast_to(whole, (NEARS, FARS, PARAM_COLS))
    return st


def last_stage(st):
    outs = [((LATENT, LANES), F32)] * 3 + [((1, LANES), F32)] * 2
    *weights, bias, gain = call(unpack_kernel, outs, (st["got"],), 1 << 18)
    st["params"] = (*weights, bias.reshape(LANES), gain.reshape(LANES))
    return st


STAGES = (
    (gather_stage, "y"),
    (send_stage, PATCH),
    (message_stage, "y"),
    (node_stage, PATCH),
    (grid_stage, "shifts"),
    (back_stage, NEAR),
    (far_stage, "z"),
    (sum_stage, "z"),
    (near_stage, NEAR),
    (last_stage, None),
)

NAMES = (
    "grid_latent",
    "mesh_latent",
    "w_source",
    "w_dest",
    "w_out",
    "edge_bias",
    "norm_gain",
    "edge_source",
    "edge_patch",
    "edge_node",
    "cotangent",
)


def shifted(x, by):
    return lax.ppermute(x, "y", [(i, (i + by) % CHANS) for i in range(CHANS)])


def on_device(*args):
    st = dict(zip(NAMES, args))
    st["chan"] = lax.axis_index("y")
    for stage, axes in STAGES:
        st = stage(st)
        if axes == "shifts":
            st["got"] = [st["sent"]] + [shifted(st["sent"], k) for k in range(1, CHANS)]
        elif axes is not None:
            st["got"] = lax.all_to_all(st["sent"], axes, 0, 0, tiled=True)
    return (st["updated"], st["grad_grid"], st["grad_mesh"], *st["params"])


def solution(mesh):
    torus = Mesh(mesh.devices.reshape(4, 16, 2, mesh.shape["chan"]), ("x", "z", "c", "y"))
    by_patch = P(PATCH, "y")
    return jax.shard_map(
        on_device,
        mesh=torus,
        in_specs=(by_patch, by_patch, P(), P(), P(), P("y"), P("y"))
        + (P(PATCH), P(PATCH, None), P(PATCH), by_patch),
        out_specs=(by_patch,) * 3 + (P(None, "y"),) * 3 + (P("y"),) * 2,
        check_vma=False,
    )
```

```python
import jax
import jax.numpy as jnp
from jax import lax
from jax.experimental import pallas as pl
from jax.experimental.pallas import tpu as pltpu
from jax.sharding import Mesh
from jax.sharding import PartitionSpec as P


NEAR = ("x", "c")
PATCH = ("x", "z", "c")
BF = jnp.bfloat16
F32 = jnp.float32

NORM_EPS = 1e-05
LANES = 128
CAP = 8
CHANS = 4
GRID = 256
MESH = 64
EDGES = 512
PATCHES = 128
LATENT = CHANS * LANES
SLOTS = PATCHES * CAP
HALF = CAP // 2 * LANES
COT_AT = GRID
MESH_AT = COT_AT + MESH
GAIN_AT = MESH_AT + MESH
PACK = GAIN_AT + 16
NEARS = 8
FARS = 16
WEIGHT_BLOCKS = LATENT // FARS
OWN_BLOCKS = 3 * WEIGHT_BLOCKS // NEARS
PARAM_COLS = (OWN_BLOCKS + 2) * LANES
VMEM_BYTES = 20 << 20
ALL_VMEM = 60 << 20


def dot(a, b, dims=((1,), (0,))):
    return lax.dot_general(a, b, (dims, ((), ())), preferred_element_type=F32)


def two_parts(v):
    high = v.astype(BF)
    return high, (v - high.astype(F32)).astype(BF)


def iota(shape, dim):
    return lax.broadcasted_iota(jnp.int32, shape, dim)


def cols(j):
    return slice(j * LANES, (j + 1) * LANES)


def call(kernel, outs, args, flops, vmem=VMEM_BYTES, **more):
    shapes = tuple(jax.ShapeDtypeStruct(s, d) for s, d in outs)
    return pl.pallas_call(
        kernel,
        out_shape=shapes,
        compiler_params=pltpu.CompilerParams(vmem_limit_bytes=vmem),
        **more,
        cost_estimate=pl.CostEstimate(flops=flops, bytes_accessed=1 << 20, transcendentals=0),
    )(*args)


def pack_kernel(grid, cot, mesh, gain, out):
    high, rest = two_parts(gain[...])
    left = gain[...] - high.astype(F32)
    low = left - rest.astype(F32)
    row = iota((16, LANES), 0)
    parts = jnp.where(
        row == 0,
        high.astype(F32),
        jnp.where(row == 1, rest.astype(F32), jnp.where(row == 2, low, 0.0)),
    )
    for j in range(CHANS):
        out[j, 0:GRID] = grid[...]
        out[j, COT_AT:MESH_AT] = cot[...]
        out[j, MESH_AT:GAIN_AT] = mesh[...]
        out[j, GAIN_AT:PACK] = parts.astype(BF)


def slot_kernel(
    patch_col, patch_row, source, node, bias, gain, pick, meta, bias_out, gain_out
):
    bias_out[...] = bias[...]
    gain_out[...] = gain[...]
    before = iota((EDGES, EDGES), 0) < iota((EDGES, EDGES), 1)
    same = patch_col[...] == patch_row[...]
    rank = jnp.sum(jnp.where(same & before, 1.0, 0.0), axis=0, keepdims=True)
    slot = rank.astype(jnp.int32) * PATCHES + patch_row[...]
    here = jnp.where(iota((SLOTS, EDGES), 0) == slot, 1.0, 0.0).astype(BF)
    row = iota((8, EDGES), 0)
    facts = jnp.where(
        row == 0, source[...], jnp.where(row == 1, node[...], jnp.where(row == 2, 1, 0))
    )
    found = dot(here, facts.astype(F32).astype(BF), ((1,), (1,)))
    live = found[:, 2:3] > 0.5
    from_row = jnp.where(live, found[:, 0:1], -1.0).astype(jnp.int32)
    pick[...] = jnp.where(iota((SLOTS, GRID), 1) == from_row, 1.0, 0.0).astype(BF)
    to_node = jnp.where(live, found[:, 1:2], float(MESH))
    lane = iota((PATCHES, LANES), 1)
    listed = jnp.zeros((PATCHES, LANES), F32)
    for r in range(CAP):
        listed = jnp.where(lane == r, to_node[r * PATCHES : (r + 1) * PATCHES], listed)
    meta[...] = listed.astype(BF)


def slot_at(r):
    at = r // (CAP // 2) * (HALF + LANES) + r % (CAP // 2) * LANES
    return slice(at, at + LANES)


def send_kernel(packed, pick, meta, source_cols, dest_cols, out, mesh_proj):
    projected = jnp.zeros((GRID, LANES), F32)
    landed = jnp.zeros((MESH, LANES), F32)
    for j in range(CHANS):
        projected += dot(packed[j, 0:GRID], source_cols[cols(j)])
        landed += dot(packed[j, MESH_AT:GAIN_AT], dest_cols[cols(j)])
    mesh_proj[...] = landed
    projected = projected.astype(BF)
    for r in range(CAP):
        rows = pick[r * PATCHES : (r + 1) * PATCHES]
        out[:, slot_at(r)] = dot(rows, projected).astype(BF)
    out[:, HALF : HALF + LANES] = meta[...]
    out[:, 2 * HALF + LANES : 2 * HALF + 2 * LANES] = jnp.zeros((PATCHES, LANES), BF)


def message_kernel(arrived, mesh_proj, bias, summed, pre, chosen):
    high, low = two_parts(mesh_proj[...])
    both = jnp.concatenate([high, low], axis=1)
    total = jnp.zeros((MESH, 2 * LANES), F32)
    for r in range(CAP):
        at = slice(r * PATCHES, (r + 1) * PATCHES)
        node = arrived[:, HALF + r : HALF + r + 1].astype(F32).astype(jnp.int32)
        mine = jnp.where(iota((PATCHES, MESH), 1) == node, 1.0, 0.0).astype(BF)
        chosen[at] = mine
        there = dot(mine, both)
        value = (
            arrived[:, slot_at(r)].astype(F32)
            + (there[:, 0:LANES] + there[:, LANES : 2 * LANES])
            + bias[...]
        )
        pre[at] = value
        message = value * jax.nn.sigmoid(value)
        total += dot(mine, jnp.concatenate(two_parts(message), axis=1), ((0,), (0,)))
    done = (total[:, 0:LANES] + total[:, LANES : 2 * LANES]).astype(BF)
    for j in range(CHANS):
        summed[j] = done


def node_kernel(
    packed,
    summed,
    pre,
    chosen,
    w_out,
    out_cols,
    out_rows,
    mesh,
    cot,
    gain,
    updated,
    grads,
    node_grad,
    dest_part,
    out_part,
    bias_part,
    gain_part,
):
    mixed = jnp.zeros((MESH, LATENT), F32)
    own = jnp.zeros((MESH, LANES), F32)
    for j in range(CHANS):
        mixed += dot(summed[j], w_out[cols(j)])
        own += dot(summed[j], out_cols[cols(j)])
    mean = jnp.sum(mixed, axis=1, keepdims=True) / LATENT
    apart = mixed - mean
    inv = lax.rsqrt(jnp.sum(apart * apart, axis=1, keepdims=True) / LATENT + NORM_EPS)
    normed = apart * inv
    scaled, first, second = [], 0.0, 0.0
    for j in range(CHANS):
        parts = packed[j, GAIN_AT:PACK].astype(F32)
        whole = parts[0:1] + parts[1:2] + parts[2:3]
        part = packed[j, COT_AT:MESH_AT].astype(F32) * whole
        scaled.append(part)
        first += jnp.sum(part, axis=1, keepdims=True)
        second += jnp.sum(part * normed[:, cols(j)], axis=1, keepdims=True)
    first, second = first / LATENT, second / LATENT
    own_normed = (own - mean) * inv
    cotangent = cot[...].astype(F32)
    updated[...] = (mesh[...].astype(F32) + own_normed * gain[...]).astype(BF)
    gain_part[...] = jnp.sum(cotangent * own_normed, axis=0, keepdims=True)
    own_grad = ((cotangent * gain[...] - first - own_normed * second) * inv).astype(BF)
    back = jnp.zeros((MESH, LANES), F32)
    for j in range(CHANS):
        out_part[cols(j)] = dot(summed[j], own_grad, ((0,), (0,))).astype(BF)
        part = ((scaled[j] - first - normed[:, cols(j)] * second) * inv).astype(BF)
        back += dot(part, out_rows[:, cols(j)], ((1,), (1,)))
    both = jnp.concatenate(two_parts(back), axis=1)
    bias = jnp.zeros((1, LANES), F32)
    total = jnp.zeros((MESH, LANES), F32)
    for r in range(CAP):
        at = slice(r * PATCHES, (r + 1) * PATCHES)
        mine = chosen[at]
        there = dot(mine, both)
        value = pre[at]
        gate = jax.nn.sigmoid(value)
        slope = gate * (1.0 + value * (1.0 - gate))
        grad = ((there[:, 0:LANES] + there[:, LANES : 2 * LANES]) * slope).astype(BF)
        grads[:, cols(r)] = grad
        bias += jnp.sum(grad.astype(F32), axis=0, keepdims=True)
        total += dot(mine, grad, ((0,), (0,)))
    bias_part[...] = bias
    total = total.astype(BF)
    node_grad[...] = total
    for j in range(CHANS):
        dest_part[cols(j)] = dot(packed[j, MESH_AT:GAIN_AT], total, ((0,), (0,))).astype(BF)


def grid_kernel(
    returned, pick, packed, node_grad, dest_part, out_part, bias_part, gain_part, out, params
):
    total = jnp.zeros((GRID, LANES), F32)
    for r in range(CAP):
        rows = pick[r * PATCHES : (r + 1) * PATCHES]
        total += dot(rows, returned[:, cols(r)], ((0,), (0,)))
    total = total.astype(BF)
    out[0:GRID] = total
    out[GRID : GRID + MESH] = node_grad[...]
    blocks = []
    for j in range(CHANS):
        part = dot(packed[j, 0:GRID], total, ((0,), (0,))).astype(BF)
        blocks += [part[b * FARS : (b + 1) * FARS] for b in range(LANES // FARS)]
    for whole in (dest_part, out_part):
        blocks += [whole[b * FARS : (b + 1) * FARS] for b in range(WEIGHT_BLOCKS)]
    for b, block in enumerate(blocks):
        params[b // OWN_BLOCKS, :, cols(b % OWN_BLOCKS)] = block
    head = iota((FARS, LANES), 0) == 0
    small = [bias_part[...], gain_part[...]] + [jnp.zeros((1, LANES), F32)] * (NEARS - 2)
    for g in range(NEARS):
        for k, part in enumerate(two_parts(small[g])):
            spread = jnp.where(head, part.astype(F32), 0.0)
            params[g, :, cols(OWN_BLOCKS + k)] = spread.astype(BF)


def join_kernel(own, other, out):
    out[0, 0:GRID] = own[0:GRID]
    out[0, GRID : GRID + MESH] = own[GRID : GRID + MESH]
    out[1, 0:GRID] = other[0:GRID]
    out[1, GRID : GRID + MESH] = other[GRID : GRID + MESH]


def back_kernel(chan, near, far, source_rows, dest_rows, cot, grad_grid, grad_mesh):
    on_grid = jnp.zeros((GRID, LANES), F32)
    on_mesh = cot[...].astype(F32)
    for k in range(CHANS):
        block = (near, far)[k // 2]
        at = pl.multiple_of(lax.bitwise_xor(chan[0], jnp.int32(k)) * LANES, LANES)
        there = pl.ds(at, LANES)
        on_grid += dot(block[k % 2, 0:GRID], source_rows[:, there], ((1,), (1,)))
        on_mesh += dot(block[k % 2, GRID : GRID + MESH], dest_rows[:, there], ((1,), (1,)))
    grad_grid[...] = on_grid.astype(BF)
    grad_mesh[...] = on_mesh.astype(BF)


def near_sum_kernel(params, out):
    total = params[0].astype(F32)
    for g in range(1, NEARS):
        total += params[g].astype(F32)
    small = total[:, cols(OWN_BLOCKS)] + total[:, cols(OWN_BLOCKS + 1)]
    out[:, 0 : OWN_BLOCKS * LANES] = total[:, 0 : OWN_BLOCKS * LANES].astype(BF)
    for k, part in enumerate(two_parts(small)):
        out[:, cols(OWN_BLOCKS + k)] = part


def unpack_kernel(params, source, dest, out, bias, gain):
    for b in range(3 * WEIGHT_BLOCKS):
        block = params[b // OWN_BLOCKS, :, cols(b % OWN_BLOCKS)].astype(F32)
        at = b % WEIGHT_BLOCKS * FARS
        (source, dest, out)[b // WEIGHT_BLOCKS][at : at + FARS] = block
    for g, small in enumerate((bias, gain)):
        high = params[g, 0:1, cols(OWN_BLOCKS)].astype(F32)
        small[...] = high + params[g, 0:1, cols(OWN_BLOCKS + 1)].astype(F32)


def gather_stage(st):
    args = (st["grid_latent"], st["cotangent"], st["mesh_latent"], st["norm_gain"][None])
    outs = [((CHANS, PACK, LANES), BF)]
    (st["sent"],) = call(pack_kernel, outs, args, 1 << 20, ALL_VMEM)
    return st


def send_stage(st):
    offset = st["chan"] * LANES
    st["packed"] = st["got"]
    for name in ("source", "dest", "out"):
        whole = st["w_" + name]
        st[name + "_cols"] = lax.dynamic_slice_in_dim(whole, offset, LANES, 1)
        st[name + "_rows"] = lax.dynamic_slice_in_dim(whole, offset, LANES, 0)
    patch = st["edge_patch"]
    args = [patch, patch.reshape(1, EDGES), st["edge_source"][None], st["edge_node"][None]]
    args += [st["edge_bias"][None], st["norm_gain"][None]]
    outs = [((SLOTS, GRID), BF), ((PATCHES, LANES), BF)] + [((1, LANES), F32)] * 2
    st["pick"], meta, st["bias"], st["gain"] = call(slot_kernel, outs, args, 1 << 27)
    args = (st["packed"], st["pick"], meta, st["source_cols"], st["dest_cols"])
    outs = [((PATCHES, 2 * HALF + 2 * LANES), BF), ((MESH, LANES), F32)]
    sent, st["mesh_proj"] = call(send_kernel, outs, args, 1 << 28)
    st["sent"] = sent.reshape(PATCHES, 2, HALF + LANES)
    return st


def message_stage(st):
    arrived = st["got"].reshape(PATCHES, 2 * HALF + 2 * LANES)
    outs = [((CHANS, MESH, LANES), BF), ((SLOTS, LANES), F32), ((SLOTS, MESH), BF)]
    args = (arrived, st["mesh_proj"], st["bias"])
    st["sent"], st["pre"], st["chosen"] = call(message_kernel, outs, args, 1 << 27)
    return st


def node_stage(st):
    args = [st["packed"], st["got"], st["pre"], st["chosen"], st["w_out"], st["out_cols"]]
    args += [st["out_rows"], st["mesh_latent"], st["cotangent"], st["gain"]]
    outs = [((MESH, LANES), BF), ((PATCHES, 2 * HALF), BF), ((MESH, LANES), BF)]
    outs += [((LATENT, LANES), BF)] * 2 + [((1, LANES), F32)] * 2
    st["updated"], grads, *st["partial"] = call(node_kernel, outs, args, 1 << 28)
    st["sent"] = grads.reshape(PATCHES, 2, HALF)
    return st


def grid_stage(st):
    returned = st["got"].reshape(PATCHES, 2 * HALF)
    outs = [((GRID + MESH, LANES), BF), ((NEARS, FARS, PARAM_COLS), BF)]
    args = (returned, st["pick"], st["packed"], *st["partial"])
    st["sent"], st["params"] = call(grid_kernel, outs, args, 1 << 28)
    return st


def join_stage(st):
    outs = [((2, GRID + MESH, LANES), BF)]
    (st["near"],) = call(join_kernel, outs, (st["sent"], st["got"]), 1 << 18)
    st["sent"] = st["near"]
    return st


def back_stage(st):
    args = (st["chan"][None], st["near"], st["got"])
    args += (st["source_rows"], st["dest_rows"], st["cotangent"])
    outs = [((GRID, LANES), BF), ((MESH, LANES), BF)]
    specs = [pl.BlockSpec(memory_space=pltpu.SMEM)] + [pl.BlockSpec()] * (len(args) - 1)
    st["grad_grid"], st["grad_mesh"] = call(back_kernel, outs, args, 1 << 26, in_specs=specs)
    st["sent"] = st["params"]
    return st


def far_stage(st):
    (sent,) = call(near_sum_kernel, [((FARS, PARAM_COLS), BF)], (st["got"],), 1 << 18)
    st["sent"] = sent.reshape(FARS, 2, PARAM_COLS // 2)
    return st


def sum_stage(st):
    total = jnp.sum(st["got"].astype(F32), axis=0)
    at = PARAM_COLS // 2 - 2 * LANES
    small = total[1:2, at : at + LANES] + total[1:2, at + LANES :]
    high = lax.reduce_precision(small, 8, 7)
    last = jnp.concatenate([total[1:2, :at], high, small - high], axis=1)
    total = jnp.concatenate([total[0:1], last], axis=0).astype(BF)
    st["sent"] = jnp.broadcast_to(total, (FARS, 2, PARAM_COLS // 2))
    return st


def near_stage(st):
    whole = st["got"].reshape(FARS, PARAM_COLS)
    st["sent"] = jnp.broadcast_to(whole, (NEARS, FARS, PARAM_COLS))
    return st


def last_stage(st):
    outs = [((LATENT, LANES), F32)] * 3 + [((1, LANES), F32)] * 2
    *weights, bias, gain = call(unpack_kernel, outs, (st["got"],), 1 << 18)
    st["params"] = (*weights, bias.reshape(LANES), gain.reshape(LANES))
    return st


STAGES = (
    (gather_stage, "y"),
    (send_stage, PATCH),
    (message_stage, "y"),
    (node_stage, PATCH),
    (grid_stage, 1),
    (join_stage, 2),
    (back_stage, NEAR),
    (far_stage, "z"),
    (sum_stage, "z"),
    (near_stage, NEAR),
    (last_stage, None),
)

NAMES = (
    "grid_latent",
    "mesh_latent",
    "w_source",
    "w_dest",
    "w_out",
    "edge_bias",
    "norm_gain",
    "edge_source",
    "edge_patch",
    "edge_node",
    "cotangent",
)


def on_device(*args):
    st = dict(zip(NAMES, args))
    st["chan"] = lax.axis_index("y")
    for stage, axes in STAGES:
        st = stage(st)
        if axes in (1, 2):
            st["got"] = lax.ppermute(st["sent"], "y", [(i, i ^ axes) for i in range(CHANS)])
        elif axes is not None:
            st["got"] = lax.all_to_all(st["sent"], axes, 0, 0, tiled=True)
    return (st["updated"], st["grad_grid"], st["grad_mesh"], *st["params"])


def solution(mesh):
    torus = Mesh(mesh.devices.reshape(4, 16, 2, mesh.shape["chan"]), ("x", "z", "c", "y"))
    by_patch = P(PATCH, "y")
    return jax.shard_map(
        on_device,
        mesh=torus,
        in_specs=(by_patch, by_patch, P(), P(), P(), P("y"), P("y"))
        + (P(PATCH), P(PATCH, None), P(PATCH), by_patch),
        out_specs=(by_patch,) * 3 + (P(None, "y"),) * 3 + (P("y"),) * 2,
        check_vma=False,
    )
```

```python
import jax
import jax.numpy as jnp
from jax import lax
from jax.experimental import pallas as pl
from jax.experimental.pallas import tpu as pltpu
from jax.sharding import Mesh
from jax.sharding import PartitionSpec as P


NEAR = ("x", "zl", "c")
PATCH = ("x", "zh", "zl", "c")
BF = jnp.bfloat16
F32 = jnp.float32

NORM_EPS = 1e-05
LANES = 128
CAP = 8
CHANS = 4
GRID = 256
MESH = 64
EDGES = 512
PATCHES = 128
LATENT = CHANS * LANES
SLOTS = PATCHES * CAP
HALF = CAP // 2 * LANES
COT_AT = GRID
MESH_AT = COT_AT + MESH
GAIN_AT = MESH_AT + MESH
PACK = GAIN_AT + 16
NEARS = 16
FARS = 8
WEIGHT_ROWS = 3 * LATENT // NEARS
OWN_ROWS = WEIGHT_ROWS + 8
BLOCK = 32
VMEM_BYTES = 20 << 20
ALL_VMEM = 60 << 20


def dot(a, b, dims=((1,), (0,))):
    return lax.dot_general(a, b, (dims, ((), ())), preferred_element_type=F32)


def two_parts(v):
    high = v.astype(BF)
    return high, (v - high.astype(F32)).astype(BF)


def iota(shape, dim):
    return lax.broadcasted_iota(jnp.int32, shape, dim)


def cols(j):
    return slice(j * LANES, (j + 1) * LANES)


def call(kernel, outs, args, flops, vmem=VMEM_BYTES, **more):
    shapes = tuple(jax.ShapeDtypeStruct(s, d) for s, d in outs)
    return pl.pallas_call(
        kernel,
        out_shape=shapes,
        compiler_params=pltpu.CompilerParams(vmem_limit_bytes=vmem),
        **more,
        cost_estimate=pl.CostEstimate(flops=flops, bytes_accessed=1 << 20, transcendentals=0),
    )(*args)


def pack_kernel(grid, cot, mesh, gain, out):
    high, rest = two_parts(gain[...])
    left = gain[...] - high.astype(F32)
    low = left - rest.astype(F32)
    row = iota((16, LANES), 0)
    parts = jnp.where(
        row == 0,
        high.astype(F32),
        jnp.where(row == 1, rest.astype(F32), jnp.where(row == 2, low, 0.0)),
    )
    for j in range(CHANS):
        out[j, 0:GRID] = grid[...]
        out[j, COT_AT:MESH_AT] = cot[...]
        out[j, MESH_AT:GAIN_AT] = mesh[...]
        out[j, GAIN_AT:PACK] = parts.astype(BF)


def slot_kernel(
    patch_col, patch_row, source, node, bias, gain, pick, meta, bias_out, gain_out
):
    bias_out[...] = bias[...]
    gain_out[...] = gain[...]
    before = iota((EDGES, EDGES), 0) < iota((EDGES, EDGES), 1)
    same = patch_col[...] == patch_row[...]
    rank = jnp.sum(jnp.where(same & before, 1.0, 0.0), axis=0, keepdims=True)
    slot = rank.astype(jnp.int32) * PATCHES + patch_row[...]
    here = jnp.where(iota((SLOTS, EDGES), 0) == slot, 1.0, 0.0).astype(BF)
    row = iota((8, EDGES), 0)
    facts = jnp.where(
        row == 0, source[...], jnp.where(row == 1, node[...], jnp.where(row == 2, 1, 0))
    )
    found = dot(here, facts.astype(F32).astype(BF), ((1,), (1,)))
    live = found[:, 2:3] > 0.5
    from_row = jnp.where(live, found[:, 0:1], -1.0).astype(jnp.int32)
    pick[...] = jnp.where(iota((SLOTS, GRID), 1) == from_row, 1.0, 0.0).astype(BF)
    to_node = jnp.where(live, found[:, 1:2], float(MESH))
    lane = iota((PATCHES, LANES), 1)
    listed = jnp.zeros((PATCHES, LANES), F32)
    for r in range(CAP):
        listed = jnp.where(lane == r, to_node[r * PATCHES : (r + 1) * PATCHES], listed)
    meta[...] = listed.astype(BF)


def slot_at(r):
    at = r // (CAP // 2) * (HALF + LANES) + r % (CAP // 2) * LANES
    return slice(at, at + LANES)


def send_kernel(packed, pick, meta, source_cols, dest_cols, out, mesh_proj):
    projected = jnp.zeros((GRID, LANES), F32)
    landed = jnp.zeros((MESH, LANES), F32)
    for j in range(CHANS):
        projected += dot(packed[j, 0:GRID], source_cols[cols(j)])
        landed += dot(packed[j, MESH_AT:GAIN_AT], dest_cols[cols(j)])
    mesh_proj[...] = landed
    projected = projected.astype(BF)
    for r in range(CAP):
        rows = pick[r * PATCHES : (r + 1) * PATCHES]
        out[:, slot_at(r)] = dot(rows, projected).astype(BF)
    out[:, HALF : HALF + LANES] = meta[...]
    out[:, 2 * HALF + LANES : 2 * HALF + 2 * LANES] = jnp.zeros((PATCHES, LANES), BF)


def message_kernel(arrived, mesh_proj, bias, summed, pre, chosen):
    high, low = two_parts(mesh_proj[...])
    both = jnp.concatenate([high, low], axis=1)
    total = jnp.zeros((MESH, 2 * LANES), F32)
    for r in range(CAP):
        at = slice(r * PATCHES, (r + 1) * PATCHES)
        node = arrived[:, HALF + r : HALF + r + 1].astype(F32).astype(jnp.int32)
        mine = jnp.where(iota((PATCHES, MESH), 1) == node, 1.0, 0.0).astype(BF)
        chosen[at] = mine
        there = dot(mine, both)
        value = (
            arrived[:, slot_at(r)].astype(F32)
            + (there[:, 0:LANES] + there[:, LANES : 2 * LANES])
            + bias[...]
        )
        pre[at] = value
        message = value * jax.nn.sigmoid(value)
        total += dot(mine, jnp.concatenate(two_parts(message), axis=1), ((0,), (0,)))
    done = (total[:, 0:LANES] + total[:, LANES : 2 * LANES]).astype(BF)
    for j in range(CHANS):
        summed[j] = done


def node_kernel(
    packed,
    summed,
    pre,
    chosen,
    w_out,
    out_cols,
    out_rows,
    mesh,
    cot,
    gain,
    updated,
    grads,
    node_grad,
    dest_part,
    out_part,
    bias_part,
    gain_part,
):
    mixed = jnp.zeros((MESH, LATENT), F32)
    own = jnp.zeros((MESH, LANES), F32)
    for j in range(CHANS):
        mixed += dot(summed[j], w_out[cols(j)])
        own += dot(summed[j], out_cols[cols(j)])
    mean = jnp.sum(mixed, axis=1, keepdims=True) / LATENT
    apart = mixed - mean
    inv = lax.rsqrt(jnp.sum(apart * apart, axis=1, keepdims=True) / LATENT + NORM_EPS)
    normed = apart * inv
    scaled, first, second = [], 0.0, 0.0
    for j in range(CHANS):
        parts = packed[j, GAIN_AT:PACK].astype(F32)
        whole = parts[0:1] + parts[1:2] + parts[2:3]
        part = packed[j, COT_AT:MESH_AT].astype(F32) * whole
        scaled.append(part)
        first += jnp.sum(part, axis=1, keepdims=True)
        second += jnp.sum(part * normed[:, cols(j)], axis=1, keepdims=True)
    first, second = first / LATENT, second / LATENT
    own_normed = (own - mean) * inv
    cotangent = cot[...].astype(F32)
    updated[...] = (mesh[...].astype(F32) + own_normed * gain[...]).astype(BF)
    gain_part[...] = jnp.sum(cotangent * own_normed, axis=0, keepdims=True)
    own_grad = ((cotangent * gain[...] - first - own_normed * second) * inv).astype(BF)
    back = jnp.zeros((MESH, LANES), F32)
    for j in range(CHANS):
        out_part[cols(j)] = dot(summed[j], own_grad, ((0,), (0,))).astype(BF)
        part = ((scaled[j] - first - normed[:, cols(j)] * second) * inv).astype(BF)
        back += dot(part, out_rows[:, cols(j)], ((1,), (1,)))
    both = jnp.concatenate(two_parts(back), axis=1)
    bias = jnp.zeros((1, LANES), F32)
    total = jnp.zeros((MESH, LANES), F32)
    for r in range(CAP):
        at = slice(r * PATCHES, (r + 1) * PATCHES)
        mine = chosen[at]
        there = dot(mine, both)
        value = pre[at]
        gate = jax.nn.sigmoid(value)
        slope = gate * (1.0 + value * (1.0 - gate))
        grad = ((there[:, 0:LANES] + there[:, LANES : 2 * LANES]) * slope).astype(BF)
        grads[:, cols(r)] = grad
        bias += jnp.sum(grad.astype(F32), axis=0, keepdims=True)
        total += dot(mine, grad, ((0,), (0,)))
    bias_part[...] = bias
    total = total.astype(BF)
    node_grad[...] = total
    for j in range(CHANS):
        dest_part[cols(j)] = dot(packed[j, MESH_AT:GAIN_AT], total, ((0,), (0,))).astype(BF)


def place(row):
    at = row % WEIGHT_ROWS
    return row // WEIGHT_ROWS, slice(at, at + BLOCK)


def small_rows(v):
    high, low = two_parts(v)
    row = iota((OWN_ROWS - WEIGHT_ROWS, LANES), 0)
    rows = jnp.where(row == 0, high.astype(F32), jnp.where(row == 1, low.astype(F32), 0.0))
    return rows.astype(BF)


def grid_kernel(
    returned, pick, packed, node_grad, dest_part, out_part, bias_part, gain_part, out, params
):
    total = jnp.zeros((GRID, LANES), F32)
    for r in range(CAP):
        rows = pick[r * PATCHES : (r + 1) * PATCHES]
        total += dot(rows, returned[:, cols(r)], ((0,), (0,)))
    total = total.astype(BF)
    out[0:GRID] = total
    out[GRID : GRID + MESH] = node_grad[...]
    for j in range(CHANS):
        part = dot(packed[j, 0:GRID], total, ((0,), (0,))).astype(BF)
        for at in range(0, LANES, BLOCK):
            g, own = place(j * LANES + at)
            params[g, own] = part[at : at + BLOCK]
    for k, whole in enumerate((dest_part, out_part)):
        for at in range(0, LATENT, BLOCK):
            g, own = place((k + 1) * LATENT + at)
            params[g, own] = whole[at : at + BLOCK]
    small = [bias_part[...], gain_part[...]] + [jnp.zeros((1, LANES), F32)] * (NEARS - 2)
    for g in range(NEARS):
        params[g, WEIGHT_ROWS:OWN_ROWS] = small_rows(small[g])


def join_kernel(own, other, out):
    out[0, 0:GRID] = own[0:GRID]
    out[0, GRID : GRID + MESH] = own[GRID : GRID + MESH]
    out[1, 0:GRID] = other[0:GRID]
    out[1, GRID : GRID + MESH] = other[GRID : GRID + MESH]


def back_kernel(chan, near, far, source_rows, dest_rows, cot, grad_grid, grad_mesh):
    on_grid = jnp.zeros((GRID, LANES), F32)
    on_mesh = cot[...].astype(F32)
    for k in range(CHANS):
        block = (near, far)[k // 2]
        at = pl.multiple_of(lax.bitwise_xor(chan[0], jnp.int32(k)) * LANES, LANES)
        there = pl.ds(at, LANES)
        on_grid += dot(block[k % 2, 0:GRID], source_rows[:, there], ((1,), (1,)))
        on_mesh += dot(block[k % 2, GRID : GRID + MESH], dest_rows[:, there], ((1,), (1,)))
    grad_grid[...] = on_grid.astype(BF)
    grad_mesh[...] = on_mesh.astype(BF)


def sum_kernel(parts, out):
    total = parts[0].astype(F32)
    for g in range(1, parts.shape[0]):
        total += parts[g].astype(F32)
    weights = total[0:WEIGHT_ROWS].astype(BF)
    small = total[WEIGHT_ROWS : WEIGHT_ROWS + 1] + total[WEIGHT_ROWS + 1 : WEIGHT_ROWS + 2]
    rows = small_rows(small)
    for g in range(out.shape[0]):
        out[g, 0:WEIGHT_ROWS] = weights
        out[g, WEIGHT_ROWS:OWN_ROWS] = rows


def unpack_kernel(params, source, dest, out, bias, gain):
    for k, whole in enumerate((source, dest, out)):
        for at in range(0, LATENT, BLOCK):
            g, own = place(k * LATENT + at)
            whole[at : at + BLOCK] = params[g, own].astype(F32)
    for g, small in enumerate((bias, gain)):
        rows = params[g, WEIGHT_ROWS:OWN_ROWS].astype(F32)
        small[...] = rows[0:1] + rows[1:2]


def gather_stage(st):
    args = (st["grid_latent"], st["cotangent"], st["mesh_latent"], st["norm_gain"][None])
    outs = [((CHANS, PACK, LANES), BF)]
    (st["sent"],) = call(pack_kernel, outs, args, 1 << 20, ALL_VMEM)
    return st


def send_stage(st):
    offset = st["chan"] * LANES
    st["packed"] = st["got"]
    for name in ("source", "dest", "out"):
        whole = st["w_" + name]
        st[name + "_cols"] = lax.dynamic_slice_in_dim(whole, offset, LANES, 1)
        st[name + "_rows"] = lax.dynamic_slice_in_dim(whole, offset, LANES, 0)
    patch = st["edge_patch"]
    args = [patch, patch.reshape(1, EDGES), st["edge_source"][None], st["edge_node"][None]]
    args += [st["edge_bias"][None], st["norm_gain"][None]]
    outs = [((SLOTS, GRID), BF), ((PATCHES, LANES), BF)] + [((1, LANES), F32)] * 2
    st["pick"], meta, st["bias"], st["gain"] = call(slot_kernel, outs, args, 1 << 27)
    args = (st["packed"], st["pick"], meta, st["source_cols"], st["dest_cols"])
    outs = [((PATCHES, 2 * HALF + 2 * LANES), BF), ((MESH, LANES), F32)]
    sent, st["mesh_proj"] = call(send_kernel, outs, args, 1 << 28)
    st["sent"] = sent.reshape(PATCHES, 2, HALF + LANES)
    return st


def message_stage(st):
    arrived = st["got"].reshape(PATCHES, 2 * HALF + 2 * LANES)
    outs = [((CHANS, MESH, LANES), BF), ((SLOTS, LANES), F32), ((SLOTS, MESH), BF)]
    args = (arrived, st["mesh_proj"], st["bias"])
    st["sent"], st["pre"], st["chosen"] = call(message_kernel, outs, args, 1 << 27)
    return st


def node_stage(st):
    args = [st["packed"], st["got"], st["pre"], st["chosen"], st["w_out"], st["out_cols"]]
    args += [st["out_rows"], st["mesh_latent"], st["cotangent"], st["gain"]]
    outs = [((MESH, LANES), BF), ((PATCHES, 2 * HALF), BF), ((MESH, LANES), BF)]
    outs += [((LATENT, LANES), BF)] * 2 + [((1, LANES), F32)] * 2
    st["updated"], grads, *st["partial"] = call(node_kernel, outs, args, 1 << 28)
    st["sent"] = grads.reshape(PATCHES, 2, HALF)
    return st


def grid_stage(st):
    returned = st["got"].reshape(PATCHES, 2 * HALF)
    outs = [((GRID + MESH, LANES), BF), ((NEARS, OWN_ROWS, LANES), BF)]
    args = (returned, st["pick"], st["packed"], *st["partial"])
    st["sent"], st["params"] = call(grid_kernel, outs, args, 1 << 28)
    return st


def join_stage(st):
    outs = [((2, GRID + MESH, LANES), BF)]
    (st["near"],) = call(join_kernel, outs, (st["sent"], st["got"]), 1 << 18)
    st["sent"] = st["near"]
    return st


def back_stage(st):
    args = (st["chan"][None], st["near"], st["got"])
    args += (st["source_rows"], st["dest_rows"], st["cotangent"])
    outs = [((GRID, LANES), BF), ((MESH, LANES), BF)]
    specs = [pl.BlockSpec(memory_space=pltpu.SMEM)] + [pl.BlockSpec()] * (len(args) - 1)
    st["grad_grid"], st["grad_mesh"] = call(back_kernel, outs, args, 1 << 26, in_specs=specs)
    st["sent"] = st["params"]
    return st


def far_stage(st):
    outs = [((FARS, OWN_ROWS, LANES), BF)]
    (st["sent"],) = call(sum_kernel, outs, (st["got"],), 1 << 20)
    return st


def near_stage(st):
    outs = [((NEARS, OWN_ROWS, LANES), BF)]
    (st["sent"],) = call(sum_kernel, outs, (st["got"],), 1 << 20)
    return st


def last_stage(st):
    outs = [((LATENT, LANES), F32)] * 3 + [((1, LANES), F32)] * 2
    *weights, bias, gain = call(unpack_kernel, outs, (st["got"],), 1 << 18)
    st["params"] = (*weights, bias.reshape(LANES), gain.reshape(LANES))
    return st


STAGES = (
    (gather_stage, "y"),
    (send_stage, PATCH),
    (message_stage, "y"),
    (node_stage, PATCH),
    (grid_stage, 1),
    (join_stage, 2),
    (back_stage, NEAR),
    (far_stage, "zh"),
    (near_stage, NEAR),
    (last_stage, None),
)

NAMES = (
    "grid_latent",
    "mesh_latent",
    "w_source",
    "w_dest",
    "w_out",
    "edge_bias",
    "norm_gain",
    "edge_source",
    "edge_patch",
    "edge_node",
    "cotangent",
)


def on_device(*args):
    st = dict(zip(NAMES, args))
    st["chan"] = lax.axis_index("y")
    for stage, axes in STAGES:
        st = stage(st)
        if axes in (1, 2):
            st["got"] = lax.ppermute(st["sent"], "y", [(i, i ^ axes) for i in range(CHANS)])
        elif axes is not None:
            st["got"] = lax.all_to_all(st["sent"], axes, 0, 0, tiled=True)
    return (st["updated"], st["grad_grid"], st["grad_mesh"], *st["params"])


def solution(mesh):
    torus = Mesh(mesh.devices.reshape(4, FARS, 2, 2, CHANS), PATCH + ("y",))
    by_patch = P(PATCH, "y")
    return jax.shard_map(
        on_device,
        mesh=torus,
        in_specs=(by_patch, by_patch, P(), P(), P(), P("y"), P("y"))
        + (P(PATCH), P(PATCH, None), P(PATCH), by_patch),
        out_specs=(by_patch,) * 3 + (P(None, "y"),) * 3 + (P("y"),) * 2,
        check_vma=False,
    )
```

```python
import jax
import jax.numpy as jnp
from jax import lax
from jax.experimental import pallas as pl
from jax.experimental.pallas import tpu as pltpu
from jax.sharding import Mesh
from jax.sharding import PartitionSpec as P


NEAR = ("x", "zl", "c")
PATCH = ("x", "zh", "zl", "c")
BF = jnp.bfloat16
F32 = jnp.float32

NORM_EPS = 1e-05
LANES = 128
CAP = 8
CHANS = 4
GRID = 256
MESH = 64
EDGES = 512
PATCHES = 128
LATENT = CHANS * LANES
SLOTS = PATCHES * CAP
HALF = CAP // 2 * LANES
COT_AT = GRID
MESH_AT = COT_AT + MESH
GAIN_AT = MESH_AT + MESH
PACK = GAIN_AT + 16
NEARS = 16
FARS = 8
WEIGHT_ROWS = 3 * LATENT // NEARS
OWN_ROWS = WEIGHT_ROWS + 8
BLOCK = 32
VMEM_BYTES = 20 << 20
ALL_VMEM = 60 << 20


def dot(a, b, dims=((1,), (0,))):
    return lax.dot_general(a, b, (dims, ((), ())), preferred_element_type=F32)


def two_parts(v):
    high = v.astype(BF)
    return high, (v - high.astype(F32)).astype(BF)


def iota(shape, dim):
    return lax.broadcasted_iota(jnp.int32, shape, dim)


def cols(j):
    return slice(j * LANES, (j + 1) * LANES)


def call(kernel, outs, args, flops, vmem=VMEM_BYTES, **more):
    shapes = tuple(jax.ShapeDtypeStruct(s, d) for s, d in outs)
    return pl.pallas_call(
        kernel,
        out_shape=shapes,
        compiler_params=pltpu.CompilerParams(vmem_limit_bytes=vmem),
        **more,
        cost_estimate=pl.CostEstimate(flops=flops, bytes_accessed=1 << 20, transcendentals=0),
    )(*args)


def scalar_first(args):
    return [pl.BlockSpec(memory_space=pltpu.SMEM)] + [pl.BlockSpec()] * (len(args) - 1)


def pack_kernel(grid, cot, mesh, gain, out):
    high, rest = two_parts(gain[...])
    left = gain[...] - high.astype(F32)
    low = left - rest.astype(F32)
    row = iota((16, LANES), 0)
    parts = jnp.where(
        row == 0,
        high.astype(F32),
        jnp.where(row == 1, rest.astype(F32), jnp.where(row == 2, low, 0.0)),
    )
    for j in range(CHANS):
        out[j, 0:GRID] = grid[...]
        out[j, COT_AT:MESH_AT] = cot[...]
        out[j, MESH_AT:GAIN_AT] = mesh[...]
        out[j, GAIN_AT:PACK] = parts.astype(BF)


def slot_kernel(chan, patch_col, patch_row, source, node, *rest):
    kept, (pick, meta, out_cols, out_rows, *copies) = rest[: len(KEPT)], rest[len(KEPT) :]
    for held, copy in zip(kept, copies):
        copy[...] = held[...]
    own = pl.ds(pl.multiple_of(chan[0] * LANES, LANES), LANES)
    out_cols[...] = kept[0][:, own]
    out_rows[...] = kept[0][own, :]
    before = iota((EDGES, EDGES), 0) < iota((EDGES, EDGES), 1)
    same = patch_col[...] == patch_row[...]
    rank = jnp.sum(jnp.where(same & before, 1.0, 0.0), axis=0, keepdims=True)
    slot = rank.astype(jnp.int32) * PATCHES + patch_row[...]
    here = jnp.where(iota((SLOTS, EDGES), 0) == slot, 1.0, 0.0).astype(BF)
    row = iota((8, EDGES), 0)
    facts = jnp.where(
        row == 0, source[...], jnp.where(row == 1, node[...], jnp.where(row == 2, 1, 0))
    )
    found = dot(here, facts.astype(F32).astype(BF), ((1,), (1,)))
    live = found[:, 2:3] > 0.5
    from_row = jnp.where(live, found[:, 0:1], -1.0).astype(jnp.int32)
    pick[...] = jnp.where(iota((SLOTS, GRID), 1) == from_row, 1.0, 0.0).astype(BF)
    to_node = jnp.where(live, found[:, 1:2], float(MESH))
    lane = iota((PATCHES, LANES), 1)
    listed = jnp.zeros((PATCHES, LANES), F32)
    for r in range(CAP):
        listed = jnp.where(lane == r, to_node[r * PATCHES : (r + 1) * PATCHES], listed)
    meta[...] = listed.astype(BF)


def slot_at(r):
    at = r // (CAP // 2) * (HALF + LANES) + r % (CAP // 2) * LANES
    return slice(at, at + LANES)


def send_kernel(packed, pick, meta, source_cols, dest_cols, out, mesh_proj):
    projected = jnp.zeros((GRID, LANES), F32)
    landed = jnp.zeros((MESH, LANES), F32)
    for j in range(CHANS):
        projected += dot(packed[j, 0:GRID], source_cols[cols(j)])
        landed += dot(packed[j, MESH_AT:GAIN_AT], dest_cols[cols(j)])
    mesh_proj[...] = landed
    projected = projected.astype(BF)
    for r in range(CAP):
        rows = pick[r * PATCHES : (r + 1) * PATCHES]
        out[:, slot_at(r)] = dot(rows, projected).astype(BF)
    out[:, HALF : HALF + LANES] = meta[...]
    out[:, 2 * HALF + LANES : 2 * HALF + 2 * LANES] = jnp.zeros((PATCHES, LANES), BF)


def message_kernel(arrived, mesh_proj, bias, summed, pre, chosen):
    high, low = two_parts(mesh_proj[...])
    both = jnp.concatenate([high, low], axis=1)
    total = jnp.zeros((MESH, 2 * LANES), F32)
    for r in range(CAP):
        at = slice(r * PATCHES, (r + 1) * PATCHES)
        node = arrived[:, HALF + r : HALF + r + 1].astype(F32).astype(jnp.int32)
        mine = jnp.where(iota((PATCHES, MESH), 1) == node, 1.0, 0.0).astype(BF)
        chosen[at] = mine
        there = dot(mine, both)
        value = (
            arrived[:, slot_at(r)].astype(F32)
            + (there[:, 0:LANES] + there[:, LANES : 2 * LANES])
            + bias[...]
        )
        pre[at] = value
        message = value * jax.nn.sigmoid(value)
        total += dot(mine, jnp.concatenate(two_parts(message), axis=1), ((0,), (0,)))
    done = (total[:, 0:LANES] + total[:, LANES : 2 * LANES]).astype(BF)
    for j in range(CHANS):
        summed[j] = done


def node_kernel(
    packed,
    summed,
    pre,
    chosen,
    w_out,
    out_cols,
    out_rows,
    mesh,
    cot,
    gain,
    updated,
    grads,
    node_grad,
    dest_part,
    out_part,
    bias_part,
    gain_part,
):
    mixed = jnp.zeros((MESH, LATENT), F32)
    own = jnp.zeros((MESH, LANES), F32)
    for j in range(CHANS):
        mixed += dot(summed[j], w_out[cols(j)])
        own += dot(summed[j], out_cols[cols(j)])
    mean = jnp.sum(mixed, axis=1, keepdims=True) / LATENT
    apart = mixed - mean
    inv = lax.rsqrt(jnp.sum(apart * apart, axis=1, keepdims=True) / LATENT + NORM_EPS)
    normed = apart * inv
    scaled, first, second = [], 0.0, 0.0
    for j in range(CHANS):
        parts = packed[j, GAIN_AT:PACK].astype(F32)
        whole = parts[0:1] + parts[1:2] + parts[2:3]
        part = packed[j, COT_AT:MESH_AT].astype(F32) * whole
        scaled.append(part)
        first += jnp.sum(part, axis=1, keepdims=True)
        second += jnp.sum(part * normed[:, cols(j)], axis=1, keepdims=True)
    first, second = first / LATENT, second / LATENT
    own_normed = (own - mean) * inv
    cotangent = cot[...].astype(F32)
    updated[...] = (mesh[...].astype(F32) + own_normed * gain[...]).astype(BF)
    gain_part[...] = jnp.sum(cotangent * own_normed, axis=0, keepdims=True)
    own_grad = ((cotangent * gain[...] - first - own_normed * second) * inv).astype(BF)
    back = jnp.zeros((MESH, LANES), F32)
    for j in range(CHANS):
        out_part[cols(j)] = dot(summed[j], own_grad, ((0,), (0,))).astype(BF)
        part = ((scaled[j] - first - normed[:, cols(j)] * second) * inv).astype(BF)
        back += dot(part, out_rows[:, cols(j)], ((1,), (1,)))
    both = jnp.concatenate(two_parts(back), axis=1)
    bias = jnp.zeros((1, LANES), F32)
    total = jnp.zeros((MESH, LANES), F32)
    for r in range(CAP):
        at = slice(r * PATCHES, (r + 1) * PATCHES)
        mine = chosen[at]
        there = dot(mine, both)
        value = pre[at]
        gate = jax.nn.sigmoid(value)
        slope = gate * (1.0 + value * (1.0 - gate))
        grad = ((there[:, 0:LANES] + there[:, LANES : 2 * LANES]) * slope).astype(BF)
        grads[:, cols(r)] = grad
        bias += jnp.sum(grad.astype(F32), axis=0, keepdims=True)
        total += dot(mine, grad, ((0,), (0,)))
    bias_part[...] = bias
    total = total.astype(BF)
    node_grad[...] = total
    for j in range(CHANS):
        dest_part[cols(j)] = dot(packed[j, MESH_AT:GAIN_AT], total, ((0,), (0,))).astype(BF)


def place(row):
    at = row % WEIGHT_ROWS
    return row // WEIGHT_ROWS, slice(at, at + BLOCK)


def small_rows(v):
    high, low = two_parts(v)
    row = iota((OWN_ROWS - WEIGHT_ROWS, LANES), 0)
    rows = jnp.where(row == 0, high.astype(F32), jnp.where(row == 1, low.astype(F32), 0.0))
    return rows.astype(BF)


def grid_kernel(
    returned, pick, packed, node_grad, dest_part, out_part, bias_part, gain_part, out, params
):
    total = jnp.zeros((GRID, LANES), F32)
    for r in range(CAP):
        rows = pick[r * PATCHES : (r + 1) * PATCHES]
        total += dot(rows, returned[:, cols(r)], ((0,), (0,)))
    total = total.astype(BF)
    out[0:GRID] = total
    out[GRID : GRID + MESH] = node_grad[...]
    for j in range(CHANS):
        part = dot(packed[j, 0:GRID], total, ((0,), (0,))).astype(BF)
        for at in range(0, LANES, BLOCK):
            g, own = place(j * LANES + at)
            params[g, own] = part[at : at + BLOCK]
    for k, whole in enumerate((dest_part, out_part)):
        for at in range(0, LATENT, BLOCK):
            g, own = place((k + 1) * LATENT + at)
            params[g, own] = whole[at : at + BLOCK]
    small = [bias_part[...], gain_part[...]] + [jnp.zeros((1, LANES), F32)] * (NEARS - 2)
    for g in range(NEARS):
        params[g, WEIGHT_ROWS:OWN_ROWS] = small_rows(small[g])


def join_kernel(own, other, out):
    out[0, 0:GRID] = own[0:GRID]
    out[0, GRID : GRID + MESH] = own[GRID : GRID + MESH]
    out[1, 0:GRID] = other[0:GRID]
    out[1, GRID : GRID + MESH] = other[GRID : GRID + MESH]


def back_kernel(chan, near, far, source_rows, dest_rows, cot, grad_grid, grad_mesh):
    on_grid = jnp.zeros((GRID, LANES), F32)
    on_mesh = cot[...].astype(F32)
    for k in range(CHANS):
        block = (near, far)[k // 2]
        at = pl.multiple_of(lax.bitwise_xor(chan[0], jnp.int32(k)) * LANES, LANES)
        there = pl.ds(at, LANES)
        on_grid += dot(block[k % 2, 0:GRID], source_rows[:, there], ((1,), (1,)))
        on_mesh += dot(block[k % 2, GRID : GRID + MESH], dest_rows[:, there], ((1,), (1,)))
    grad_grid[...] = on_grid.astype(BF)
    grad_mesh[...] = on_mesh.astype(BF)


def sum_kernel(parts, out):
    total = parts[0].astype(F32)
    for g in range(1, parts.shape[0]):
        total += parts[g].astype(F32)
    weights = total[0:WEIGHT_ROWS].astype(BF)
    small = total[WEIGHT_ROWS : WEIGHT_ROWS + 1] + total[WEIGHT_ROWS + 1 : WEIGHT_ROWS + 2]
    rows = small_rows(small)
    for g in range(out.shape[0]):
        out[g, 0:WEIGHT_ROWS] = weights
        out[g, WEIGHT_ROWS:OWN_ROWS] = rows


def unpack_kernel(params, source, dest, out, bias, gain):
    for k, whole in enumerate((source, dest, out)):
        for at in range(0, LATENT, BLOCK):
            g, own = place(k * LATENT + at)
            whole[at : at + BLOCK] = params[g, own].astype(F32)
    for g, small in enumerate((bias, gain)):
        rows = params[g, WEIGHT_ROWS:OWN_ROWS].astype(F32)
        small[...] = rows[0:1] + rows[1:2]


KEPT = ("w_out", "edge_bias", "norm_gain", "mesh_latent", "cotangent")


def gather_stage(st):
    args = (st["grid_latent"], st["cotangent"], st["mesh_latent"], st["norm_gain"][None])
    outs = [((CHANS, PACK, LANES), BF)]
    (st["sent"],) = call(pack_kernel, outs, args, 1 << 20, ALL_VMEM)
    return st


def send_stage(st):
    offset = st["chan"] * LANES
    st["packed"] = st["got"]
    for name in ("source", "dest"):
        whole = st["w_" + name]
        st[name + "_cols"] = lax.dynamic_slice_in_dim(whole, offset, LANES, 1)
        st[name + "_rows"] = lax.dynamic_slice_in_dim(whole, offset, LANES, 0)
    patch = st["edge_patch"]
    args = [patch, patch.reshape(1, EDGES), st["edge_source"][None], st["edge_node"][None]]
    kept = [st[name].reshape(-1, st[name].shape[-1]) for name in KEPT]
    outs = [((SLOTS, GRID), BF), ((PATCHES, LANES), BF), ((LATENT, LANES), BF)]
    outs += [((LANES, LATENT), BF)] + [(v.shape, v.dtype) for v in kept]
    args = [st["chan"][None]] + args + kept
    results = call(slot_kernel, outs, args, 1 << 27, in_specs=scalar_first(args))
    st["pick"], meta, st["out_cols"], st["out_rows"], *copies = results
    st["kept"] = dict(zip(KEPT, copies))
    args = (st["packed"], st["pick"], meta, st["source_cols"], st["dest_cols"])
    outs = [((PATCHES, 2 * HALF + 2 * LANES), BF), ((MESH, LANES), F32)]
    sent, st["mesh_proj"] = call(send_kernel, outs, args, 1 << 28)
    st["sent"] = sent.reshape(PATCHES, 2, HALF + LANES)
    return st


def message_stage(st):
    arrived = st["got"].reshape(PATCHES, 2 * HALF + 2 * LANES)
    outs = [((CHANS, MESH, LANES), BF), ((SLOTS, LANES), F32), ((SLOTS, MESH), BF)]
    args = (arrived, st["mesh_proj"], st["kept"]["edge_bias"])
    st["sent"], st["pre"], st["chosen"] = call(message_kernel, outs, args, 1 << 27)
    return st


def node_stage(st):
    kept = st["kept"]
    args = [st["packed"], st["got"], st["pre"], st["chosen"], kept["w_out"], st["out_cols"]]
    args += [st["out_rows"], kept["mesh_latent"], kept["cotangent"], kept["norm_gain"]]
    outs = [((MESH, LANES), BF), ((PATCHES, 2 * HALF), BF), ((MESH, LANES), BF)]
    outs += [((LATENT, LANES), BF)] * 2 + [((1, LANES), F32)] * 2
    st["updated"], grads, *st["partial"] = call(node_kernel, outs, args, 1 << 28)
    st["sent"] = grads.reshape(PATCHES, 2, HALF)
    return st


def grid_stage(st):
    returned = st["got"].reshape(PATCHES, 2 * HALF)
    outs = [((GRID + MESH, LANES), BF), ((NEARS, OWN_ROWS, LANES), BF)]
    args = (returned, st["pick"], st["packed"], *st["partial"])
    st["sent"], st["params"] = call(grid_kernel, outs, args, 1 << 28)
    return st


def join_stage(st):
    outs = [((2, GRID + MESH, LANES), BF)]
    (st["near"],) = call(join_kernel, outs, (st["sent"], st["got"]), 1 << 18)
    st["sent"] = st["near"]
    return st


def back_stage(st):
    args = (st["chan"][None], st["near"], st["got"])
    args += (st["source_rows"], st["dest_rows"], st["kept"]["cotangent"])
    outs = [((GRID, LANES), BF), ((MESH, LANES), BF)]
    specs = scalar_first(args)
    st["grad_grid"], st["grad_mesh"] = call(back_kernel, outs, args, 1 << 26, in_specs=specs)
    st["sent"] = st["params"]
    return st


def far_stage(st):
    outs = [((FARS, OWN_ROWS, LANES), BF)]
    (st["sent"],) = call(sum_kernel, outs, (st["got"],), 1 << 20)
    return st


def near_stage(st):
    outs = [((NEARS, OWN_ROWS, LANES), BF)]
    (st["sent"],) = call(sum_kernel, outs, (st["got"],), 1 << 20)
    return st


def last_stage(st):
    outs = [((LATENT, LANES), F32)] * 3 + [((1, LANES), F32)] * 2
    *weights, bias, gain = call(unpack_kernel, outs, (st["got"],), 1 << 18)
    st["params"] = (*weights, bias.reshape(LANES), gain.reshape(LANES))
    return st


STAGES = (
    (gather_stage, "y"),
    (send_stage, PATCH),
    (message_stage, "y"),
    (node_stage, PATCH),
    (grid_stage, 1),
    (join_stage, 2),
    (back_stage, NEAR),
    (far_stage, "zh"),
    (near_stage, NEAR),
    (last_stage, None),
)

NAMES = (
    "grid_latent",
    "mesh_latent",
    "w_source",
    "w_dest",
    "w_out",
    "edge_bias",
    "norm_gain",
    "edge_source",
    "edge_patch",
    "edge_node",
    "cotangent",
)


def on_device(*args):
    st = dict(zip(NAMES, args))
    st["chan"] = lax.axis_index("y")
    for stage, axes in STAGES:
        st = stage(st)
        if axes in (1, 2):
            st["got"] = lax.ppermute(st["sent"], "y", [(i, i ^ axes) for i in range(CHANS)])
        elif axes is not None:
            st["got"] = lax.all_to_all(st["sent"], axes, 0, 0, tiled=True)
    return (st["updated"], st["grad_grid"], st["grad_mesh"], *st["params"])


def solution(mesh):
    torus = Mesh(mesh.devices.reshape(4, FARS, 2, 2, CHANS), PATCH + ("y",))
    by_patch = P(PATCH, "y")
    return jax.shard_map(
        on_device,
        mesh=torus,
        in_specs=(by_patch, by_patch, P(), P(), P(), P("y"), P("y"))
        + (P(PATCH), P(PATCH, None), P(PATCH), by_patch),
        out_specs=(by_patch,) * 3 + (P(None, "y"),) * 3 + (P("y"),) * 2,
        check_vma=False,
    )
```

```python
import jax
import jax.numpy as jnp
from jax import lax
from jax.experimental import pallas as pl
from jax.experimental.pallas import tpu as pltpu
from jax.sharding import Mesh
from jax.sharding import PartitionSpec as P


NEAR = ("x", "zl", "c")
PATCH = ("x", "zh", "zl", "c")
BF = jnp.bfloat16
F32 = jnp.float32

NORM_EPS = 1e-05
LANES = 128
CAP = 8
CHANS = 4
GRID = 256
MESH = 64
EDGES = 512
PATCHES = 128
LATENT = CHANS * LANES
SLOTS = PATCHES * CAP
HALF = CAP // 2 * LANES
COT_AT = GRID
MESH_AT = COT_AT + MESH
GAIN_AT = MESH_AT + MESH
PACK = GAIN_AT + 16
NEARS = 16
FARS = 8
WEIGHT_ROWS = 3 * LATENT // NEARS
OWN_ROWS = WEIGHT_ROWS + 8
BLOCK = 32
VMEM_BYTES = 20 << 20
ALL_VMEM = 60 << 20


def dot(a, b, dims=((1,), (0,))):
    return lax.dot_general(a, b, (dims, ((), ())), preferred_element_type=F32)


def two_parts(v):
    high = v.astype(BF)
    return high, (v - high.astype(F32)).astype(BF)


def iota(shape, dim):
    return lax.broadcasted_iota(jnp.int32, shape, dim)


def joined(blocks):
    return jnp.concatenate(blocks, axis=1)


def cols(j):
    return slice(j * LANES, (j + 1) * LANES)


def call(kernel, outs, args, flops, vmem=VMEM_BYTES, **more):
    shapes = tuple(jax.ShapeDtypeStruct(s, d) for s, d in outs)
    return pl.pallas_call(
        kernel,
        out_shape=shapes,
        compiler_params=pltpu.CompilerParams(vmem_limit_bytes=vmem),
        **more,
        cost_estimate=pl.CostEstimate(flops=flops, bytes_accessed=1 << 20, transcendentals=0),
    )(*args)


def scalar_first(args):
    return [pl.BlockSpec(memory_space=pltpu.SMEM)] + [pl.BlockSpec()] * (len(args) - 1)


def pack_kernel(grid, cot, mesh, gain, out):
    high, rest = two_parts(gain[...])
    left = gain[...] - high.astype(F32)
    low = left - rest.astype(F32)
    row = iota((16, LANES), 0)
    parts = jnp.where(
        row == 0,
        high.astype(F32),
        jnp.where(row == 1, rest.astype(F32), jnp.where(row == 2, low, 0.0)),
    )
    for j in range(CHANS):
        out[j, 0:GRID] = grid[...]
        out[j, COT_AT:MESH_AT] = cot[...]
        out[j, MESH_AT:GAIN_AT] = mesh[...]
        out[j, GAIN_AT:PACK] = parts.astype(BF)


def slot_kernel(chan, patch_col, patch_row, source, node, *rest):
    kept, (pick, meta, out_cols, out_rows, *copies) = rest[: len(KEPT)], rest[len(KEPT) :]
    for held, copy in zip(kept, copies):
        copy[...] = held[...]
    own = pl.ds(pl.multiple_of(chan[0] * LANES, LANES), LANES)
    out_cols[...] = kept[0][:, own]
    out_rows[...] = kept[0][own, :]
    before = iota((EDGES, EDGES), 0) < iota((EDGES, EDGES), 1)
    same = patch_col[...] == patch_row[...]
    rank = jnp.sum(jnp.where(same & before, 1.0, 0.0), axis=0, keepdims=True)
    slot = rank.astype(jnp.int32) * PATCHES + patch_row[...]
    here = jnp.where(iota((SLOTS, EDGES), 0) == slot, 1.0, 0.0).astype(BF)
    row = iota((8, EDGES), 0)
    facts = jnp.where(
        row == 0, source[...], jnp.where(row == 1, node[...], jnp.where(row == 2, 1, 0))
    )
    found = dot(here, facts.astype(F32).astype(BF), ((1,), (1,)))
    live = found[:, 2:3] > 0.5
    from_row = jnp.where(live, found[:, 0:1], -1.0).astype(jnp.int32)
    pick[...] = jnp.where(iota((SLOTS, GRID), 1) == from_row, 1.0, 0.0).astype(BF)
    to_node = jnp.where(live, found[:, 1:2], float(MESH))
    lane = iota((PATCHES, LANES), 1)
    listed = jnp.zeros((PATCHES, LANES), F32)
    for r in range(CAP):
        listed = jnp.where(lane == r, to_node[r * PATCHES : (r + 1) * PATCHES], listed)
    meta[...] = listed.astype(BF)


def slot_at(r):
    at = r // (CAP // 2) * (HALF + LANES) + r % (CAP // 2) * LANES
    return slice(at, at + LANES)


def send_kernel(packed, pick, meta, source_cols, dest_cols, out, mesh_proj):
    projected = jnp.zeros((GRID, LANES), F32)
    landed = jnp.zeros((MESH, LANES), F32)
    for j in range(CHANS):
        projected += dot(packed[j, 0:GRID], source_cols[cols(j)])
        landed += dot(packed[j, MESH_AT:GAIN_AT], dest_cols[cols(j)])
    mesh_proj[...] = landed
    projected = projected.astype(BF)
    for r in range(CAP):
        rows = pick[r * PATCHES : (r + 1) * PATCHES]
        out[:, slot_at(r)] = dot(rows, projected).astype(BF)
    out[:, HALF : HALF + LANES] = meta[...]
    out[:, 2 * HALF + LANES : 2 * HALF + 2 * LANES] = jnp.zeros((PATCHES, LANES), BF)


def message_kernel(arrived, mesh_proj, bias, summed, pre, chosen):
    high, low = two_parts(mesh_proj[...])
    both = jnp.concatenate([high, low], axis=1)
    total = jnp.zeros((MESH, 2 * LANES), F32)
    for r in range(CAP):
        at = slice(r * PATCHES, (r + 1) * PATCHES)
        node = arrived[:, HALF + r : HALF + r + 1].astype(F32).astype(jnp.int32)
        mine = jnp.where(iota((PATCHES, MESH), 1) == node, 1.0, 0.0).astype(BF)
        chosen[at] = mine
        there = dot(mine, both)
        value = (
            arrived[:, slot_at(r)].astype(F32)
            + (there[:, 0:LANES] + there[:, LANES : 2 * LANES])
            + bias[...]
        )
        pre[at] = value
        message = value * jax.nn.sigmoid(value)
        total += dot(mine, jnp.concatenate(two_parts(message), axis=1), ((0,), (0,)))
    done = (total[:, 0:LANES] + total[:, LANES : 2 * LANES]).astype(BF)
    for j in range(CHANS):
        summed[j] = done


def node_kernel(
    packed,
    summed,
    pre,
    chosen,
    w_out,
    out_cols,
    out_rows,
    mesh,
    cot,
    gain,
    updated,
    grads,
    node_grad,
    dest_part,
    out_part,
    bias_part,
    gain_part,
):
    whole = joined([summed[j] for j in range(CHANS)])
    mixed = dot(whole, w_out[...])
    own = dot(whole, out_cols[...])
    mean = jnp.sum(mixed, axis=1, keepdims=True) / LATENT
    apart = mixed - mean
    inv = lax.rsqrt(jnp.sum(apart * apart, axis=1, keepdims=True) / LATENT + NORM_EPS)
    normed = apart * inv
    parts = joined([packed[j, GAIN_AT:PACK] for j in range(CHANS)]).astype(F32)
    scaled = joined([packed[j, COT_AT:MESH_AT] for j in range(CHANS)]).astype(F32)
    scaled = scaled * (parts[0:1] + parts[1:2] + parts[2:3])
    first = jnp.sum(scaled, axis=1, keepdims=True) / LATENT
    second = jnp.sum(scaled * normed, axis=1, keepdims=True) / LATENT
    part = ((scaled - first - normed * second) * inv).astype(BF)
    back = dot(part, out_rows[...], ((1,), (1,)))
    there = dot(chosen[...], joined(two_parts(back)))
    value = pre[...]
    gate = jax.nn.sigmoid(value)
    slope = gate * (1.0 + value * (1.0 - gate))
    grad = ((there[:, 0:LANES] + there[:, LANES : 2 * LANES]) * slope).astype(BF)
    for r in range(CAP):
        grads[:, cols(r)] = grad[r * PATCHES : (r + 1) * PATCHES]
    bias_part[...] = jnp.sum(grad.astype(F32), axis=0, keepdims=True)
    total = dot(chosen[...], grad, ((0,), (0,))).astype(BF)
    node_grad[...] = total
    nodes = joined([packed[j, MESH_AT:GAIN_AT] for j in range(CHANS)])
    dest_part[...] = dot(nodes, total, ((0,), (0,))).astype(BF)
    own_normed = (own - mean) * inv
    cotangent = cot[...].astype(F32)
    updated[...] = (mesh[...].astype(F32) + own_normed * gain[...]).astype(BF)
    gain_part[...] = jnp.sum(cotangent * own_normed, axis=0, keepdims=True)
    own_grad = ((cotangent * gain[...] - first - own_normed * second) * inv).astype(BF)
    out_part[...] = dot(whole, own_grad, ((0,), (0,))).astype(BF)


def place(row):
    at = row % WEIGHT_ROWS
    return row // WEIGHT_ROWS, slice(at, at + BLOCK)


def small_rows(v):
    high, low = two_parts(v)
    row = iota((OWN_ROWS - WEIGHT_ROWS, LANES), 0)
    rows = jnp.where(row == 0, high.astype(F32), jnp.where(row == 1, low.astype(F32), 0.0))
    return rows.astype(BF)


def grid_kernel(
    returned, pick, packed, node_grad, dest_part, out_part, bias_part, gain_part, out, params
):
    total = jnp.zeros((GRID, LANES), F32)
    for r in range(CAP):
        rows = pick[r * PATCHES : (r + 1) * PATCHES]
        total += dot(rows, returned[:, cols(r)], ((0,), (0,)))
    total = total.astype(BF)
    out[0:GRID] = total
    out[GRID : GRID + MESH] = node_grad[...]
    for j in range(CHANS):
        part = dot(packed[j, 0:GRID], total, ((0,), (0,))).astype(BF)
        for at in range(0, LANES, BLOCK):
            g, own = place(j * LANES + at)
            params[g, own] = part[at : at + BLOCK]
    for k, whole in enumerate((dest_part, out_part)):
        for at in range(0, LATENT, BLOCK):
            g, own = place((k + 1) * LATENT + at)
            params[g, own] = whole[at : at + BLOCK]
    small = [bias_part[...], gain_part[...]] + [jnp.zeros((1, LANES), F32)] * (NEARS - 2)
    for g in range(NEARS):
        params[g, WEIGHT_ROWS:OWN_ROWS] = small_rows(small[g])


def join_kernel(own, other, out):
    out[0, 0:GRID] = own[0:GRID]
    out[0, GRID : GRID + MESH] = own[GRID : GRID + MESH]
    out[1, 0:GRID] = other[0:GRID]
    out[1, GRID : GRID + MESH] = other[GRID : GRID + MESH]


def back_kernel(chan, near, far, source_rows, dest_rows, cot, grad_grid, grad_mesh):
    on_grid = jnp.zeros((GRID, LANES), F32)
    on_mesh = cot[...].astype(F32)
    for k in range(CHANS):
        block = (near, far)[k // 2]
        other = lax.bitwise_xor(chan[0], jnp.int32((0, 2, 1, 3)[k]))
        at = pl.multiple_of(other * LANES, LANES)
        there = pl.ds(at, LANES)
        on_grid += dot(block[k % 2, 0:GRID], source_rows[:, there], ((1,), (1,)))
        on_mesh += dot(block[k % 2, GRID : GRID + MESH], dest_rows[:, there], ((1,), (1,)))
    grad_grid[...] = on_grid.astype(BF)
    grad_mesh[...] = on_mesh.astype(BF)


def sum_kernel(parts, out):
    total = parts[0].astype(F32)
    for g in range(1, parts.shape[0]):
        total += parts[g].astype(F32)
    weights = total[0:WEIGHT_ROWS].astype(BF)
    small = total[WEIGHT_ROWS : WEIGHT_ROWS + 1] + total[WEIGHT_ROWS + 1 : WEIGHT_ROWS + 2]
    rows = small_rows(small)
    for g in range(out.shape[0]):
        out[g, 0:WEIGHT_ROWS] = weights
        out[g, WEIGHT_ROWS:OWN_ROWS] = rows


def unpack_kernel(params, source, dest, out, bias, gain):
    for k, whole in enumerate((source, dest, out)):
        for at in range(0, LATENT, BLOCK):
            g, own = place(k * LATENT + at)
            whole[at : at + BLOCK] = params[g, own].astype(F32)
    for g, small in enumerate((bias, gain)):
        rows = params[g, WEIGHT_ROWS:OWN_ROWS].astype(F32)
        small[...] = rows[0:1] + rows[1:2]


KEPT = ("w_out", "edge_bias", "norm_gain", "mesh_latent", "cotangent")


def gather_stage(st):
    args = (st["grid_latent"], st["cotangent"], st["mesh_latent"], st["norm_gain"][None])
    outs = [((CHANS, PACK, LANES), BF)]
    (st["sent"],) = call(pack_kernel, outs, args, 1 << 20, ALL_VMEM)
    return st


def send_stage(st):
    offset = st["chan"] * LANES
    st["packed"] = st["got"]
    for name in ("source", "dest"):
        whole = st["w_" + name]
        st[name + "_cols"] = lax.dynamic_slice_in_dim(whole, offset, LANES, 1)
        st[name + "_rows"] = lax.dynamic_slice_in_dim(whole, offset, LANES, 0)
    patch = st["edge_patch"]
    args = [patch, patch.reshape(1, EDGES), st["edge_source"][None], st["edge_node"][None]]
    kept = [st[name].reshape(-1, st[name].shape[-1]) for name in KEPT]
    outs = [((SLOTS, GRID), BF), ((PATCHES, LANES), BF), ((LATENT, LANES), BF)]
    outs += [((LANES, LATENT), BF)] + [(v.shape, v.dtype) for v in kept]
    args = [st["chan"][None]] + args + kept
    results = call(slot_kernel, outs, args, 1 << 27, in_specs=scalar_first(args))
    st["pick"], meta, st["out_cols"], st["out_rows"], *copies = results
    st["kept"] = dict(zip(KEPT, copies))
    args = (st["packed"], st["pick"], meta, st["source_cols"], st["dest_cols"])
    outs = [((PATCHES, 2 * HALF + 2 * LANES), BF), ((MESH, LANES), F32)]
    sent, st["mesh_proj"] = call(send_kernel, outs, args, 1 << 28)
    st["sent"] = sent.reshape(PATCHES, 2, HALF + LANES)
    return st


def message_stage(st):
    arrived = st["got"].reshape(PATCHES, 2 * HALF + 2 * LANES)
    outs = [((CHANS, MESH, LANES), BF), ((SLOTS, LANES), F32), ((SLOTS, MESH), BF)]
    args = (arrived, st["mesh_proj"], st["kept"]["edge_bias"])
    st["sent"], st["pre"], st["chosen"] = call(message_kernel, outs, args, 1 << 27)
    return st


def node_stage(st):
    kept = st["kept"]
    args = [st["packed"], st["got"], st["pre"], st["chosen"], kept["w_out"], st["out_cols"]]
    args += [st["out_rows"], kept["mesh_latent"], kept["cotangent"], kept["norm_gain"]]
    outs = [((MESH, LANES), BF), ((PATCHES, 2 * HALF), BF), ((MESH, LANES), BF)]
    outs += [((LATENT, LANES), BF)] * 2 + [((1, LANES), F32)] * 2
    st["updated"], grads, *st["partial"] = call(node_kernel, outs, args, 1 << 28)
    st["sent"] = grads.reshape(PATCHES, 2, HALF)
    return st


def grid_stage(st):
    returned = st["got"].reshape(PATCHES, 2 * HALF)
    outs = [((GRID + MESH, LANES), BF), ((NEARS, OWN_ROWS, LANES), BF)]
    args = (returned, st["pick"], st["packed"], *st["partial"])
    st["sent"], st["params"] = call(grid_kernel, outs, args, 1 << 28)
    return st


def join_stage(st):
    outs = [((2, GRID + MESH, LANES), BF)]
    (st["near"],) = call(join_kernel, outs, (st["sent"], st["got"]), 1 << 18)
    st["sent"] = st["near"]
    return st


def back_stage(st):
    args = (st["chan"][None], st["near"], st["got"])
    args += (st["source_rows"], st["dest_rows"], st["kept"]["cotangent"])
    outs = [((GRID, LANES), BF), ((MESH, LANES), BF)]
    specs = scalar_first(args)
    st["grad_grid"], st["grad_mesh"] = call(back_kernel, outs, args, 1 << 26, in_specs=specs)
    st["sent"] = st["params"]
    return st


def far_stage(st):
    outs = [((FARS, OWN_ROWS, LANES), BF)]
    (st["sent"],) = call(sum_kernel, outs, (st["got"],), 1 << 20)
    return st


def near_stage(st):
    outs = [((NEARS, OWN_ROWS, LANES), BF)]
    (st["sent"],) = call(sum_kernel, outs, (st["got"],), 1 << 20)
    return st


def last_stage(st):
    outs = [((LATENT, LANES), F32)] * 3 + [((1, LANES), F32)] * 2
    *weights, bias, gain = call(unpack_kernel, outs, (st["got"],), 1 << 18)
    st["params"] = (*weights, bias.reshape(LANES), gain.reshape(LANES))
    return st


STAGES = (
    (gather_stage, "y"),
    (send_stage, PATCH),
    (message_stage, "y"),
    (node_stage, PATCH),
    (grid_stage, 2),
    (join_stage, 1),
    (back_stage, NEAR),
    (far_stage, "zh"),
    (near_stage, NEAR),
    (last_stage, None),
)

NAMES = (
    "grid_latent",
    "mesh_latent",
    "w_source",
    "w_dest",
    "w_out",
    "edge_bias",
    "norm_gain",
    "edge_source",
    "edge_patch",
    "edge_node",
    "cotangent",
)


def on_device(*args):
    st = dict(zip(NAMES, args))
    st["chan"] = lax.axis_index("y")
    for stage, axes in STAGES:
        st = stage(st)
        if axes in (1, 2):
            st["got"] = lax.ppermute(st["sent"], "y", [(i, i ^ axes) for i in range(CHANS)])
        elif axes is not None:
            st["got"] = lax.all_to_all(st["sent"], axes, 0, 0, tiled=True)
    return (st["updated"], st["grad_grid"], st["grad_mesh"], *st["params"])


def solution(mesh):
    torus = Mesh(mesh.devices.reshape(4, FARS, 2, 2, CHANS), PATCH + ("y",))
    by_patch = P(PATCH, "y")
    return jax.shard_map(
        on_device,
        mesh=torus,
        in_specs=(by_patch, by_patch, P(), P(), P(), P("y"), P("y"))
        + (P(PATCH), P(PATCH, None), P(PATCH), by_patch),
        out_specs=(by_patch,) * 3 + (P(None, "y"),) * 3 + (P("y"),) * 2,
        check_vma=False,
    )
```

```python
import jax
import jax.numpy as jnp
from jax import lax
from jax.experimental import pallas as pl
from jax.experimental.pallas import tpu as pltpu
from jax.sharding import Mesh
from jax.sharding import PartitionSpec as P


NEAR = ("x", "zl", "c")
PATCH = ("x", "zh", "zl", "c")
BF = jnp.bfloat16
F32 = jnp.float32

NORM_EPS = 1e-05
LANES = 128
CAP = 8
CHANS = 4
GRID = 256
MESH = 64
EDGES = 512
PATCHES = 128
LATENT = CHANS * LANES
SLOTS = PATCHES * CAP
HALF = CAP // 2 * LANES
COT_AT = GRID
MESH_AT = COT_AT + MESH
GAIN_AT = MESH_AT + MESH
PACK = GAIN_AT + 16
NEARS = 16
FARS = 8
WEIGHT_ROWS = 3 * LATENT // NEARS
OWN_ROWS = WEIGHT_ROWS + 8
BLOCK = 32
VMEM_BYTES = 20 << 20
ALL_VMEM = 60 << 20


def dot(a, b, dims=((1,), (0,))):
    return lax.dot_general(a, b, (dims, ((), ())), preferred_element_type=F32)


def two_parts(v):
    high = v.astype(BF)
    return high, (v - high.astype(F32)).astype(BF)


def iota(shape, dim):
    return lax.broadcasted_iota(jnp.int32, shape, dim)


def joined(blocks):
    return jnp.concatenate(blocks, axis=1)


def cols(j):
    return slice(j * LANES, (j + 1) * LANES)


def call(kernel, outs, args, flops, vmem=VMEM_BYTES, **more):
    shapes = tuple(jax.ShapeDtypeStruct(s, d) for s, d in outs)
    return pl.pallas_call(
        kernel,
        out_shape=shapes,
        compiler_params=pltpu.CompilerParams(vmem_limit_bytes=vmem),
        **more,
        cost_estimate=pl.CostEstimate(flops=flops, bytes_accessed=1 << 20, transcendentals=0),
    )(*args)


def scalar_first(args):
    return [pl.BlockSpec(memory_space=pltpu.SMEM)] + [pl.BlockSpec()] * (len(args) - 1)


def pack_kernel(grid, cot, mesh, gain, out):
    high, rest = two_parts(gain[...])
    left = gain[...] - high.astype(F32)
    low = left - rest.astype(F32)
    row = iota((16, LANES), 0)
    parts = jnp.where(
        row == 0,
        high.astype(F32),
        jnp.where(row == 1, rest.astype(F32), jnp.where(row == 2, low, 0.0)),
    )
    for j in range(CHANS):
        out[j, 0:GRID] = grid[...]
        out[j, COT_AT:MESH_AT] = cot[...]
        out[j, MESH_AT:GAIN_AT] = mesh[...]
        out[j, GAIN_AT:PACK] = parts.astype(BF)


def slot_kernel(chan, patch_col, patch_row, source, node, *rest):
    kept, (pick, meta, out_cols, out_rows, *copies) = rest[: len(KEPT)], rest[len(KEPT) :]
    for held, copy in zip(kept, copies):
        copy[...] = held[...]
    own = pl.ds(pl.multiple_of(chan[0] * LANES, LANES), LANES)
    out_cols[...] = kept[0][:, own]
    out_rows[...] = kept[0][own, :]
    before = iota((EDGES, EDGES), 0) < iota((EDGES, EDGES), 1)
    same = patch_col[...] == patch_row[...]
    rank = jnp.sum(jnp.where(same & before, 1.0, 0.0), axis=0, keepdims=True)
    slot = rank.astype(jnp.int32) * PATCHES + patch_row[...]
    here = jnp.where(iota((SLOTS, EDGES), 0) == slot, 1.0, 0.0).astype(BF)
    row = iota((8, EDGES), 0)
    facts = jnp.where(
        row == 0, source[...], jnp.where(row == 1, node[...], jnp.where(row == 2, 1, 0))
    )
    found = dot(here, facts.astype(F32).astype(BF), ((1,), (1,)))
    live = found[:, 2:3] > 0.5
    from_row = jnp.where(live, found[:, 0:1], -1.0).astype(jnp.int32)
    pick[...] = jnp.where(iota((SLOTS, GRID), 1) == from_row, 1.0, 0.0).astype(BF)
    to_node = jnp.where(live, found[:, 1:2], float(MESH))
    lane = iota((PATCHES, LANES), 1)
    listed = jnp.zeros((PATCHES, LANES), F32)
    for r in range(CAP):
        listed = jnp.where(lane == r, to_node[r * PATCHES : (r + 1) * PATCHES], listed)
    meta[...] = listed.astype(BF)


def slot_at(r):
    at = r // (CAP // 2) * (HALF + LANES) + r % (CAP // 2) * LANES
    return slice(at, at + LANES)


def send_kernel(packed, pick, meta, source_cols, dest_cols, out, mesh_proj):
    projected = jnp.zeros((GRID, LANES), F32)
    landed = jnp.zeros((MESH, LANES), F32)
    for j in range(CHANS):
        projected += dot(packed[j, 0:GRID], source_cols[cols(j)])
        landed += dot(packed[j, MESH_AT:GAIN_AT], dest_cols[cols(j)])
    mesh_proj[...] = landed
    projected = projected.astype(BF)
    for r in range(CAP):
        rows = pick[r * PATCHES : (r + 1) * PATCHES]
        out[:, slot_at(r)] = dot(rows, projected).astype(BF)
    out[:, HALF : HALF + LANES] = meta[...]
    out[:, 2 * HALF + LANES : 2 * HALF + 2 * LANES] = jnp.zeros((PATCHES, LANES), BF)


def message_kernel(arrived, mesh_proj, bias, summed, pre, chosen):
    high, low = two_parts(mesh_proj[...])
    both = jnp.concatenate([high, low], axis=1)
    total = jnp.zeros((MESH, 2 * LANES), F32)
    for r in range(CAP):
        at = slice(r * PATCHES, (r + 1) * PATCHES)
        node = arrived[:, HALF + r : HALF + r + 1].astype(F32).astype(jnp.int32)
        mine = jnp.where(iota((PATCHES, MESH), 1) == node, 1.0, 0.0).astype(BF)
        chosen[at] = mine
        there = dot(mine, both)
        value = (
            arrived[:, slot_at(r)].astype(F32)
            + (there[:, 0:LANES] + there[:, LANES : 2 * LANES])
            + bias[...]
        )
        pre[at] = value
        message = value * jax.nn.sigmoid(value)
        total += dot(mine, jnp.concatenate(two_parts(message), axis=1), ((0,), (0,)))
    done = (total[:, 0:LANES] + total[:, LANES : 2 * LANES]).astype(BF)
    for j in range(CHANS):
        summed[j] = done


def node_kernel(
    packed,
    summed,
    pre,
    chosen,
    w_out,
    out_cols,
    out_rows,
    mesh,
    cot,
    gain,
    updated,
    grads,
    node_grad,
    dest_part,
    out_part,
    bias_part,
    gain_part,
):
    whole = joined([summed[j] for j in range(CHANS)])
    mixed = dot(whole, w_out[...])
    own = dot(whole, out_cols[...])
    mean = jnp.sum(mixed, axis=1, keepdims=True) / LATENT
    apart = mixed - mean
    inv = lax.rsqrt(jnp.sum(apart * apart, axis=1, keepdims=True) / LATENT + NORM_EPS)
    normed = apart * inv
    parts = joined([packed[j, GAIN_AT:PACK] for j in range(CHANS)]).astype(F32)
    scaled = joined([packed[j, COT_AT:MESH_AT] for j in range(CHANS)]).astype(F32)
    scaled = scaled * (parts[0:1] + parts[1:2] + parts[2:3])
    first = jnp.sum(scaled, axis=1, keepdims=True) / LATENT
    second = jnp.sum(scaled * normed, axis=1, keepdims=True) / LATENT
    part = ((scaled - first - normed * second) * inv).astype(BF)
    back = dot(part, out_rows[...], ((1,), (1,)))
    there = dot(chosen[...], joined(two_parts(back)))
    value = pre[...]
    gate = jax.nn.sigmoid(value)
    slope = gate * (1.0 + value * (1.0 - gate))
    grad = ((there[:, 0:LANES] + there[:, LANES : 2 * LANES]) * slope).astype(BF)
    for r in range(CAP):
        grads[:, cols(r)] = grad[r * PATCHES : (r + 1) * PATCHES]
    bias_part[...] = jnp.sum(grad.astype(F32), axis=0, keepdims=True)
    total = dot(chosen[...], grad, ((0,), (0,))).astype(BF)
    node_grad[...] = total
    nodes = joined([packed[j, MESH_AT:GAIN_AT] for j in range(CHANS)])
    dest_part[...] = dot(nodes, total, ((0,), (0,))).astype(BF)
    own_normed = (own - mean) * inv
    cotangent = cot[...].astype(F32)
    updated[...] = (mesh[...].astype(F32) + own_normed * gain[...]).astype(BF)
    gain_part[...] = jnp.sum(cotangent * own_normed, axis=0, keepdims=True)
    own_grad = ((cotangent * gain[...] - first - own_normed * second) * inv).astype(BF)
    out_part[...] = dot(whole, own_grad, ((0,), (0,))).astype(BF)


def place(row):
    at = row % WEIGHT_ROWS
    return row // WEIGHT_ROWS, slice(at, at + BLOCK)


def small_rows(v):
    high, low = two_parts(v)
    row = iota((OWN_ROWS - WEIGHT_ROWS, LANES), 0)
    rows = jnp.where(row == 0, high.astype(F32), jnp.where(row == 1, low.astype(F32), 0.0))
    return rows.astype(BF)


def grid_kernel(
    returned, pick, packed, node_grad, dest_part, out_part, bias_part, gain_part, out, params
):
    total = jnp.zeros((GRID, LANES), F32)
    for r in range(CAP):
        rows = pick[r * PATCHES : (r + 1) * PATCHES]
        total += dot(rows, returned[:, cols(r)], ((0,), (0,)))
    total = total.astype(BF)
    out[0:GRID] = total
    out[GRID : GRID + MESH] = node_grad[...]
    for j in range(CHANS):
        part = dot(packed[j, 0:GRID], total, ((0,), (0,))).astype(BF)
        for at in range(0, LANES, BLOCK):
            g, own = place(j * LANES + at)
            params[g, own] = part[at : at + BLOCK]
    for k, whole in enumerate((dest_part, out_part)):
        for at in range(0, LATENT, BLOCK):
            g, own = place((k + 1) * LATENT + at)
            params[g, own] = whole[at : at + BLOCK]
    small = [bias_part[...], gain_part[...]] + [jnp.zeros((1, LANES), F32)] * (NEARS - 2)
    for g in range(NEARS):
        params[g, WEIGHT_ROWS:OWN_ROWS] = small_rows(small[g])


def join_kernel(own, other, out):
    out[0, 0:GRID] = own[0:GRID]
    out[0, GRID : GRID + MESH] = own[GRID : GRID + MESH]
    out[1, 0:GRID] = other[0:GRID]
    out[1, GRID : GRID + MESH] = other[GRID : GRID + MESH]


def back_kernel(chan, near, far, source_rows, dest_rows, cot, grad_grid, grad_mesh):
    on_grid = jnp.zeros((GRID, LANES), F32)
    on_mesh = cot[...].astype(F32)
    for k in range(CHANS):
        block = (near, far)[k // 2]
        other = lax.bitwise_xor(chan[0], jnp.int32((0, 1, 3, 2)[k]))
        at = pl.multiple_of(other * LANES, LANES)
        there = pl.ds(at, LANES)
        on_grid += dot(block[k % 2, 0:GRID], source_rows[:, there], ((1,), (1,)))
        on_mesh += dot(block[k % 2, GRID : GRID + MESH], dest_rows[:, there], ((1,), (1,)))
    grad_grid[...] = on_grid.astype(BF)
    grad_mesh[...] = on_mesh.astype(BF)


def sum_kernel(parts, out):
    total = parts[0].astype(F32)
    for g in range(1, parts.shape[0]):
        total += parts[g].astype(F32)
    weights = total[0:WEIGHT_ROWS].astype(BF)
    small = total[WEIGHT_ROWS : WEIGHT_ROWS + 1] + total[WEIGHT_ROWS + 1 : WEIGHT_ROWS + 2]
    rows = small_rows(small)
    for g in range(out.shape[0]):
        out[g, 0:WEIGHT_ROWS] = weights
        out[g, WEIGHT_ROWS:OWN_ROWS] = rows


def unpack_kernel(params, source, dest, out, bias, gain):
    for k, whole in enumerate((source, dest, out)):
        for at in range(0, LATENT, BLOCK):
            g, own = place(k * LATENT + at)
            whole[at : at + BLOCK] = params[g, own].astype(F32)
    for g, small in enumerate((bias, gain)):
        rows = params[g, WEIGHT_ROWS:OWN_ROWS].astype(F32)
        small[...] = rows[0:1] + rows[1:2]


KEPT = ("w_out", "edge_bias", "norm_gain", "mesh_latent", "cotangent")


def gather_stage(st):
    args = (st["grid_latent"], st["cotangent"], st["mesh_latent"], st["norm_gain"][None])
    outs = [((CHANS, PACK, LANES), BF)]
    (st["sent"],) = call(pack_kernel, outs, args, 1 << 20, ALL_VMEM)
    return st


def send_stage(st):
    offset = st["chan"] * LANES
    st["packed"] = st["got"]
    for name in ("source", "dest"):
        whole = st["w_" + name]
        st[name + "_cols"] = lax.dynamic_slice_in_dim(whole, offset, LANES, 1)
        st[name + "_rows"] = lax.dynamic_slice_in_dim(whole, offset, LANES, 0)
    patch = st["edge_patch"]
    args = [patch, patch.reshape(1, EDGES), st["edge_source"][None], st["edge_node"][None]]
    kept = [st[name].reshape(-1, st[name].shape[-1]) for name in KEPT]
    outs = [((SLOTS, GRID), BF), ((PATCHES, LANES), BF), ((LATENT, LANES), BF)]
    outs += [((LANES, LATENT), BF)] + [(v.shape, v.dtype) for v in kept]
    args = [st["chan"][None]] + args + kept
    results = call(slot_kernel, outs, args, 1 << 27, in_specs=scalar_first(args))
    st["pick"], meta, st["out_cols"], st["out_rows"], *copies = results
    st["kept"] = dict(zip(KEPT, copies))
    args = (st["packed"], st["pick"], meta, st["source_cols"], st["dest_cols"])
    outs = [((PATCHES, 2 * HALF + 2 * LANES), BF), ((MESH, LANES), F32)]
    sent, st["mesh_proj"] = call(send_kernel, outs, args, 1 << 28)
    st["sent"] = sent.reshape(PATCHES, 2, HALF + LANES)
    return st


def message_stage(st):
    arrived = st["got"].reshape(PATCHES, 2 * HALF + 2 * LANES)
    outs = [((CHANS, MESH, LANES), BF), ((SLOTS, LANES), F32), ((SLOTS, MESH), BF)]
    args = (arrived, st["mesh_proj"], st["kept"]["edge_bias"])
    st["sent"], st["pre"], st["chosen"] = call(message_kernel, outs, args, 1 << 27)
    return st


def node_stage(st):
    kept = st["kept"]
    args = [st["packed"], st["got"], st["pre"], st["chosen"], kept["w_out"], st["out_cols"]]
    args += [st["out_rows"], kept["mesh_latent"], kept["cotangent"], kept["norm_gain"]]
    outs = [((MESH, LANES), BF), ((PATCHES, 2 * HALF), BF), ((MESH, LANES), BF)]
    outs += [((LATENT, LANES), BF)] * 2 + [((1, LANES), F32)] * 2
    st["updated"], grads, *st["partial"] = call(node_kernel, outs, args, 1 << 28)
    st["sent"] = grads.reshape(PATCHES, 2, HALF)
    return st


def grid_stage(st):
    returned = st["got"].reshape(PATCHES, 2 * HALF)
    outs = [((GRID + MESH, LANES), BF), ((NEARS, OWN_ROWS, LANES), BF)]
    args = (returned, st["pick"], st["packed"], *st["partial"])
    st["sent"], st["params"] = call(grid_kernel, outs, args, 1 << 28)
    return st


def join_stage(st):
    outs = [((2, GRID + MESH, LANES), BF)]
    (st["near"],) = call(join_kernel, outs, (st["sent"], st["got"]), 1 << 18)
    st["sent"] = st["near"]
    return st


def back_stage(st):
    args = (st["chan"][None], st["near"], st["got"])
    args += (st["source_rows"], st["dest_rows"], st["kept"]["cotangent"])
    outs = [((GRID, LANES), BF), ((MESH, LANES), BF)]
    specs = scalar_first(args)
    st["grad_grid"], st["grad_mesh"] = call(back_kernel, outs, args, 1 << 26, in_specs=specs)
    st["sent"] = st["params"]
    return st


def far_stage(st):
    outs = [((FARS, OWN_ROWS, LANES), BF)]
    (st["sent"],) = call(sum_kernel, outs, (st["got"],), 1 << 20)
    return st


def near_stage(st):
    outs = [((NEARS, OWN_ROWS, LANES), BF)]
    (st["sent"],) = call(sum_kernel, outs, (st["got"],), 1 << 20)
    return st


def last_stage(st):
    outs = [((LATENT, LANES), F32)] * 3 + [((1, LANES), F32)] * 2
    *weights, bias, gain = call(unpack_kernel, outs, (st["got"],), 1 << 18)
    st["params"] = (*weights, bias.reshape(LANES), gain.reshape(LANES))
    return st


STAGES = (
    (gather_stage, "y"),
    (send_stage, PATCH),
    (message_stage, "y"),
    (node_stage, PATCH),
    (grid_stage, 1),
    (join_stage, 3),
    (back_stage, NEAR),
    (far_stage, "zh"),
    (near_stage, NEAR),
    (last_stage, None),
)

NAMES = (
    "grid_latent",
    "mesh_latent",
    "w_source",
    "w_dest",
    "w_out",
    "edge_bias",
    "norm_gain",
    "edge_source",
    "edge_patch",
    "edge_node",
    "cotangent",
)


def on_device(*args):
    st = dict(zip(NAMES, args))
    st["chan"] = lax.axis_index("y")
    for stage, axes in STAGES:
        st = stage(st)
        if axes in (1, 3):
            st["got"] = lax.ppermute(st["sent"], "y", [(i, i ^ axes) for i in range(CHANS)])
        elif axes is not None:
            st["got"] = lax.all_to_all(st["sent"], axes, 0, 0, tiled=True)
    return (st["updated"], st["grad_grid"], st["grad_mesh"], *st["params"])


def solution(mesh):
    torus = Mesh(mesh.devices.reshape(4, FARS, 2, 2, CHANS), PATCH + ("y",))
    by_patch = P(PATCH, "y")
    return jax.shard_map(
        on_device,
        mesh=torus,
        in_specs=(by_patch, by_patch, P(), P(), P(), P("y"), P("y"))
        + (P(PATCH), P(PATCH, None), P(PATCH), by_patch),
        out_specs=(by_patch,) * 3 + (P(None, "y"),) * 3 + (P("y"),) * 2,
        check_vma=False,
    )
```

```python
import jax
import jax.numpy as jnp
from jax import lax
from jax.experimental import pallas as pl
from jax.experimental.pallas import tpu as pltpu
from jax.sharding import Mesh
from jax.sharding import PartitionSpec as P


NEAR = ("x", "zl", "c")
PATCH = ("x", "zh", "zl", "c")
PEERS = ("zh", "zl", "c", "x")
BF = jnp.bfloat16
F32 = jnp.float32

NORM_EPS = 1e-05
LANES = 128
CAP = 8
CHANS = 4
GRID = 256
MESH = 64
EDGES = 512
PATCHES = 128
LATENT = CHANS * LANES
SLOTS = PATCHES * CAP
HALF = CAP // 2 * LANES
COT_AT = GRID
MESH_AT = COT_AT + MESH
GAIN_AT = MESH_AT + MESH
PACK = GAIN_AT + 16
NEARS = 16
FARS = 8
WEIGHT_ROWS = 3 * LATENT // NEARS
OWN_ROWS = WEIGHT_ROWS + 8
BLOCK = 32
VMEM_BYTES = 20 << 20
ALL_VMEM = 60 << 20


def dot(a, b, dims=((1,), (0,))):
    return lax.dot_general(a, b, (dims, ((), ())), preferred_element_type=F32)


def two_parts(v):
    high = v.astype(BF)
    return high, (v - high.astype(F32)).astype(BF)


def iota(shape, dim):
    return lax.broadcasted_iota(jnp.int32, shape, dim)


def joined(blocks):
    return jnp.concatenate(blocks, axis=1)


def cols(j):
    return slice(j * LANES, (j + 1) * LANES)


def call(kernel, outs, args, flops, vmem=VMEM_BYTES, **more):
    shapes = tuple(jax.ShapeDtypeStruct(s, d) for s, d in outs)
    return pl.pallas_call(
        kernel,
        out_shape=shapes,
        compiler_params=pltpu.CompilerParams(vmem_limit_bytes=vmem),
        **more,
        cost_estimate=pl.CostEstimate(flops=flops, bytes_accessed=1 << 20, transcendentals=0),
    )(*args)


def scalar_first(args):
    return [pl.BlockSpec(memory_space=pltpu.SMEM)] + [pl.BlockSpec()] * (len(args) - 1)


def pack_kernel(grid, cot, mesh, gain, out):
    high, rest = two_parts(gain[...])
    left = gain[...] - high.astype(F32)
    low = left - rest.astype(F32)
    row = iota((16, LANES), 0)
    parts = jnp.where(
        row == 0,
        high.astype(F32),
        jnp.where(row == 1, rest.astype(F32), jnp.where(row == 2, low, 0.0)),
    )
    for j in range(CHANS):
        out[j, 0:GRID] = grid[...]
        out[j, COT_AT:MESH_AT] = cot[...]
        out[j, MESH_AT:GAIN_AT] = mesh[...]
        out[j, GAIN_AT:PACK] = parts.astype(BF)


def slot_kernel(chan, patch_col, patch_row, source, node, *rest):
    kept, (pick, meta, out_cols, out_rows, *copies) = rest[: len(KEPT)], rest[len(KEPT) :]
    for held, copy in zip(kept, copies):
        copy[...] = held[...]
    own = pl.ds(pl.multiple_of(chan[0] * LANES, LANES), LANES)
    out_cols[...] = kept[0][:, own]
    out_rows[...] = kept[0][own, :]
    before = iota((EDGES, EDGES), 0) < iota((EDGES, EDGES), 1)
    same = patch_col[...] == patch_row[...]
    rank = jnp.sum(jnp.where(same & before, 1.0, 0.0), axis=0, keepdims=True)
    peer = lax.rem(patch_row[...], PATCHES // 4) * 4 + patch_row[...] // (PATCHES // 4)
    slot = rank.astype(jnp.int32) * PATCHES + peer
    here = jnp.where(iota((SLOTS, EDGES), 0) == slot, 1.0, 0.0).astype(BF)
    row = iota((8, EDGES), 0)
    facts = jnp.where(
        row == 0, source[...], jnp.where(row == 1, node[...], jnp.where(row == 2, 1, 0))
    )
    found = dot(here, facts.astype(F32).astype(BF), ((1,), (1,)))
    live = found[:, 2:3] > 0.5
    from_row = jnp.where(live, found[:, 0:1], -1.0).astype(jnp.int32)
    pick[...] = jnp.where(iota((SLOTS, GRID), 1) == from_row, 1.0, 0.0).astype(BF)
    to_node = jnp.where(live, found[:, 1:2], float(MESH))
    lane = iota((PATCHES, LANES), 1)
    listed = jnp.zeros((PATCHES, LANES), F32)
    for r in range(CAP):
        listed = jnp.where(lane == r, to_node[r * PATCHES : (r + 1) * PATCHES], listed)
    meta[...] = listed.astype(BF)


def slot_at(r):
    at = r // (CAP // 2) * (HALF + LANES) + r % (CAP // 2) * LANES
    return slice(at, at + LANES)


def send_kernel(packed, pick, meta, source_cols, dest_cols, out, mesh_proj):
    projected = jnp.zeros((GRID, LANES), F32)
    landed = jnp.zeros((MESH, LANES), F32)
    for j in range(CHANS):
        projected += dot(packed[j, 0:GRID], source_cols[cols(j)])
        landed += dot(packed[j, MESH_AT:GAIN_AT], dest_cols[cols(j)])
    mesh_proj[...] = landed
    projected = projected.astype(BF)
    for r in range(CAP):
        rows = pick[r * PATCHES : (r + 1) * PATCHES]
        out[:, slot_at(r)] = dot(rows, projected).astype(BF)
    out[:, HALF : HALF + LANES] = meta[...]
    out[:, 2 * HALF + LANES : 2 * HALF + 2 * LANES] = jnp.zeros((PATCHES, LANES), BF)


def message_kernel(arrived, mesh_proj, bias, summed, pre, chosen):
    high, low = two_parts(mesh_proj[...])
    both = jnp.concatenate([high, low], axis=1)
    total = jnp.zeros((MESH, 2 * LANES), F32)
    for r in range(CAP):
        at = slice(r * PATCHES, (r + 1) * PATCHES)
        node = arrived[:, HALF + r : HALF + r + 1].astype(F32).astype(jnp.int32)
        mine = jnp.where(iota((PATCHES, MESH), 1) == node, 1.0, 0.0).astype(BF)
        chosen[at] = mine
        there = dot(mine, both)
        value = (
            arrived[:, slot_at(r)].astype(F32)
            + (there[:, 0:LANES] + there[:, LANES : 2 * LANES])
            + bias[...]
        )
        pre[at] = value
        message = value * jax.nn.sigmoid(value)
        total += dot(mine, jnp.concatenate(two_parts(message), axis=1), ((0,), (0,)))
    done = (total[:, 0:LANES] + total[:, LANES : 2 * LANES]).astype(BF)
    for j in range(CHANS):
        summed[j] = done


def node_kernel(
    packed,
    summed,
    pre,
    chosen,
    w_out,
    out_cols,
    out_rows,
    mesh,
    cot,
    gain,
    updated,
    grads,
    node_grad,
    dest_part,
    out_part,
    bias_part,
    gain_part,
):
    whole = joined([summed[j] for j in range(CHANS)])
    mixed = dot(whole, w_out[...])
    own = dot(whole, out_cols[...])
    mean = jnp.sum(mixed, axis=1, keepdims=True) / LATENT
    apart = mixed - mean
    inv = lax.rsqrt(jnp.sum(apart * apart, axis=1, keepdims=True) / LATENT + NORM_EPS)
    normed = apart * inv
    parts = joined([packed[j, GAIN_AT:PACK] for j in range(CHANS)]).astype(F32)
    scaled = joined([packed[j, COT_AT:MESH_AT] for j in range(CHANS)]).astype(F32)
    scaled = scaled * (parts[0:1] + parts[1:2] + parts[2:3])
    first = jnp.sum(scaled, axis=1, keepdims=True) / LATENT
    second = jnp.sum(scaled * normed, axis=1, keepdims=True) / LATENT
    part = ((scaled - first - normed * second) * inv).astype(BF)
    back = dot(part, out_rows[...], ((1,), (1,)))
    there = dot(chosen[...], joined(two_parts(back)))
    value = pre[...]
    gate = jax.nn.sigmoid(value)
    slope = gate * (1.0 + value * (1.0 - gate))
    grad = ((there[:, 0:LANES] + there[:, LANES : 2 * LANES]) * slope).astype(BF)
    for r in range(CAP):
        grads[:, cols(r)] = grad[r * PATCHES : (r + 1) * PATCHES]
    bias_part[...] = jnp.sum(grad.astype(F32), axis=0, keepdims=True)
    total = dot(chosen[...], grad, ((0,), (0,))).astype(BF)
    node_grad[...] = total
    nodes = joined([packed[j, MESH_AT:GAIN_AT] for j in range(CHANS)])
    dest_part[...] = dot(nodes, total, ((0,), (0,))).astype(BF)
    own_normed = (own - mean) * inv
    cotangent = cot[...].astype(F32)
    updated[...] = (mesh[...].astype(F32) + own_normed * gain[...]).astype(BF)
    gain_part[...] = jnp.sum(cotangent * own_normed, axis=0, keepdims=True)
    own_grad = ((cotangent * gain[...] - first - own_normed * second) * inv).astype(BF)
    out_part[...] = dot(whole, own_grad, ((0,), (0,))).astype(BF)


def place(row):
    at = row % WEIGHT_ROWS
    return row // WEIGHT_ROWS, slice(at, at + BLOCK)


def small_rows(v):
    high, low = two_parts(v)
    row = iota((OWN_ROWS - WEIGHT_ROWS, LANES), 0)
    rows = jnp.where(row == 0, high.astype(F32), jnp.where(row == 1, low.astype(F32), 0.0))
    return rows.astype(BF)


def grid_kernel(
    returned, pick, packed, node_grad, dest_part, out_part, bias_part, gain_part, out, params
):
    total = jnp.zeros((GRID, LANES), F32)
    for r in range(CAP):
        rows = pick[r * PATCHES : (r + 1) * PATCHES]
        total += dot(rows, returned[:, cols(r)], ((0,), (0,)))
    total = total.astype(BF)
    out[0:GRID] = total
    out[GRID : GRID + MESH] = node_grad[...]
    for j in range(CHANS):
        part = dot(packed[j, 0:GRID], total, ((0,), (0,))).astype(BF)
        for at in range(0, LANES, BLOCK):
            g, own = place(j * LANES + at)
            params[g, own] = part[at : at + BLOCK]
    for k, whole in enumerate((dest_part, out_part)):
        for at in range(0, LATENT, BLOCK):
            g, own = place((k + 1) * LATENT + at)
            params[g, own] = whole[at : at + BLOCK]
    small = [bias_part[...], gain_part[...]] + [jnp.zeros((1, LANES), F32)] * (NEARS - 2)
    for g in range(NEARS):
        params[g, WEIGHT_ROWS:OWN_ROWS] = small_rows(small[g])


def join_kernel(own, other, out):
    out[0, 0:GRID] = own[0:GRID]
    out[0, GRID : GRID + MESH] = own[GRID : GRID + MESH]
    out[1, 0:GRID] = other[0:GRID]
    out[1, GRID : GRID + MESH] = other[GRID : GRID + MESH]


def back_kernel(chan, near, far, source_rows, dest_rows, cot, grad_grid, grad_mesh):
    on_grid = jnp.zeros((GRID, LANES), F32)
    on_mesh = cot[...].astype(F32)
    for k in range(CHANS):
        block = (near, far)[k // 2]
        other = lax.bitwise_xor(chan[0], jnp.int32((0, 1, 3, 2)[k]))
        at = pl.multiple_of(other * LANES, LANES)
        there = pl.ds(at, LANES)
        on_grid += dot(block[k % 2, 0:GRID], source_rows[:, there], ((1,), (1,)))
        on_mesh += dot(block[k % 2, GRID : GRID + MESH], dest_rows[:, there], ((1,), (1,)))
    grad_grid[...] = on_grid.astype(BF)
    grad_mesh[...] = on_mesh.astype(BF)


def sum_kernel(parts, out):
    total = parts[0].astype(F32)
    for g in range(1, parts.shape[0]):
        total += parts[g].astype(F32)
    weights = total[0:WEIGHT_ROWS].astype(BF)
    small = total[WEIGHT_ROWS : WEIGHT_ROWS + 1] + total[WEIGHT_ROWS + 1 : WEIGHT_ROWS + 2]
    rows = small_rows(small)
    for g in range(out.shape[0]):
        out[g, 0:WEIGHT_ROWS] = weights
        out[g, WEIGHT_ROWS:OWN_ROWS] = rows


def unpack_kernel(params, source, dest, out, bias, gain):
    for k, whole in enumerate((source, dest, out)):
        for at in range(0, LATENT, BLOCK):
            g, own = place(k * LATENT + at)
            whole[at : at + BLOCK] = params[g, own].astype(F32)
    for g, small in enumerate((bias, gain)):
        rows = params[g, WEIGHT_ROWS:OWN_ROWS].astype(F32)
        small[...] = rows[0:1] + rows[1:2]


KEPT = ("w_out", "edge_bias", "norm_gain", "mesh_latent", "cotangent")


def gather_stage(st):
    args = (st["grid_latent"], st["cotangent"], st["mesh_latent"], st["norm_gain"][None])
    outs = [((CHANS, PACK, LANES), BF)]
    (st["sent"],) = call(pack_kernel, outs, args, 1 << 20, ALL_VMEM)
    return st


def send_stage(st):
    offset = st["chan"] * LANES
    st["packed"] = st["got"]
    for name in ("source", "dest"):
        whole = st["w_" + name]
        st[name + "_cols"] = lax.dynamic_slice_in_dim(whole, offset, LANES, 1)
        st[name + "_rows"] = lax.dynamic_slice_in_dim(whole, offset, LANES, 0)
    patch = st["edge_patch"]
    args = [patch, patch.reshape(1, EDGES), st["edge_source"][None], st["edge_node"][None]]
    kept = [st[name].reshape(-1, st[name].shape[-1]) for name in KEPT]
    outs = [((SLOTS, GRID), BF), ((PATCHES, LANES), BF), ((LATENT, LANES), BF)]
    outs += [((LANES, LATENT), BF)] + [(v.shape, v.dtype) for v in kept]
    args = [st["chan"][None]] + args + kept
    results = call(slot_kernel, outs, args, 1 << 27, in_specs=scalar_first(args))
    st["pick"], meta, st["out_cols"], st["out_rows"], *copies = results
    st["kept"] = dict(zip(KEPT, copies))
    args = (st["packed"], st["pick"], meta, st["source_cols"], st["dest_cols"])
    outs = [((PATCHES, 2 * HALF + 2 * LANES), BF), ((MESH, LANES), F32)]
    sent, st["mesh_proj"] = call(send_kernel, outs, args, 1 << 28)
    st["sent"] = sent.reshape(PATCHES, 2, HALF + LANES)
    return st


def message_stage(st):
    arrived = st["got"].reshape(PATCHES, 2 * HALF + 2 * LANES)
    outs = [((CHANS, MESH, LANES), BF), ((SLOTS, LANES), F32), ((SLOTS, MESH), BF)]
    args = (arrived, st["mesh_proj"], st["kept"]["edge_bias"])
    st["sent"], st["pre"], st["chosen"] = call(message_kernel, outs, args, 1 << 27)
    return st


def node_stage(st):
    kept = st["kept"]
    args = [st["packed"], st["got"], st["pre"], st["chosen"], kept["w_out"], st["out_cols"]]
    args += [st["out_rows"], kept["mesh_latent"], kept["cotangent"], kept["norm_gain"]]
    outs = [((MESH, LANES), BF), ((PATCHES, 2 * HALF), BF), ((MESH, LANES), BF)]
    outs += [((LATENT, LANES), BF)] * 2 + [((1, LANES), F32)] * 2
    st["updated"], grads, *st["partial"] = call(node_kernel, outs, args, 1 << 28)
    st["sent"] = grads.reshape(PATCHES, 2, HALF)
    return st


def grid_stage(st):
    returned = st["got"].reshape(PATCHES, 2 * HALF)
    outs = [((GRID + MESH, LANES), BF), ((NEARS, OWN_ROWS, LANES), BF)]
    args = (returned, st["pick"], st["packed"], *st["partial"])
    st["sent"], st["params"] = call(grid_kernel, outs, args, 1 << 28)
    return st


def join_stage(st):
    outs = [((2, GRID + MESH, LANES), BF)]
    (st["near"],) = call(join_kernel, outs, (st["sent"], st["got"]), 1 << 18)
    st["sent"] = st["near"]
    return st


def back_stage(st):
    args = (st["chan"][None], st["near"], st["got"])
    args += (st["source_rows"], st["dest_rows"], st["kept"]["cotangent"])
    outs = [((GRID, LANES), BF), ((MESH, LANES), BF)]
    specs = scalar_first(args)
    st["grad_grid"], st["grad_mesh"] = call(back_kernel, outs, args, 1 << 26, in_specs=specs)
    st["sent"] = st["params"]
    return st


def far_stage(st):
    outs = [((FARS, OWN_ROWS, LANES), BF)]
    (st["sent"],) = call(sum_kernel, outs, (st["got"],), 1 << 20)
    return st


def near_stage(st):
    outs = [((NEARS, OWN_ROWS, LANES), BF)]
    (st["sent"],) = call(sum_kernel, outs, (st["got"],), 1 << 20)
    return st


def last_stage(st):
    outs = [((LATENT, LANES), F32)] * 3 + [((1, LANES), F32)] * 2
    *weights, bias, gain = call(unpack_kernel, outs, (st["got"],), 1 << 18)
    st["params"] = (*weights, bias.reshape(LANES), gain.reshape(LANES))
    return st


STAGES = (
    (gather_stage, "y"),
    (send_stage, PEERS),
    (message_stage, "y"),
    (node_stage, PEERS),
    (grid_stage, 1),
    (join_stage, 3),
    (back_stage, NEAR),
    (far_stage, "zh"),
    (near_stage, NEAR),
    (last_stage, None),
)

NAMES = (
    "grid_latent",
    "mesh_latent",
    "w_source",
    "w_dest",
    "w_out",
    "edge_bias",
    "norm_gain",
    "edge_source",
    "edge_patch",
    "edge_node",
    "cotangent",
)


def on_device(*args):
    st = dict(zip(NAMES, args))
    st["chan"] = lax.axis_index("y")
    for stage, axes in STAGES:
        st = stage(st)
        if axes in (1, 3):
            st["got"] = lax.ppermute(st["sent"], "y", [(i, i ^ axes) for i in range(CHANS)])
        elif axes is not None:
            st["got"] = lax.all_to_all(st["sent"], axes, 0, 0, tiled=True)
    return (st["updated"], st["grad_grid"], st["grad_mesh"], *st["params"])


def solution(mesh):
    torus = Mesh(mesh.devices.reshape(4, FARS, 2, 2, CHANS), PATCH + ("y",))
    by_patch = P(PATCH, "y")
    return jax.shard_map(
        on_device,
        mesh=torus,
        in_specs=(by_patch, by_patch, P(), P(), P(), P("y"), P("y"))
        + (P(PATCH), P(PATCH, None), P(PATCH), by_patch),
        out_specs=(by_patch,) * 3 + (P(None, "y"),) * 3 + (P("y"),) * 2,
        check_vma=False,
    )
```
